256 devices in a mesh: dom: 128 (over x, z, y), feat: 2 (over core).
Axes of the slice: x: 4, y: 4, z: 8, core: 2. Of those that a mesh axis runs over, the one named last changes fastest.
Arguments:
- features: bfloat16 [131072, 512], P('dom', 'feat'), may hold values from -6 to 6
- grad_out: bfloat16 [131072, 512], P('dom', 'feat'), may hold values from -6 to 6
- pre_act: bfloat16 [131072, 512], P('dom', 'feat'), may hold values from -6 to 6
- neigh_mean: bfloat16 [131072, 512], P('dom', 'feat'), may hold values from -6 to 6
- w_self: bfloat16 [512, 512], P('feat'), may hold values from -0.25 to 0.25
- w_neigh: bfloat16 [512, 512], P('feat'), may hold values from -0.25 to 0.25
- edge_from: int32 [1048576], P('dom'), may hold values from 0 to 5119
- edge_to: int32 [1048576], P('dom'), may hold values from 0 to 5119
- edge_count: int32 [128], P('dom'), may hold values from 2048 to 8192, as said below
- mirror_master: int32 [524288], P('dom'), may hold values from 0 to 63
- degrees: int32 [131072], P('dom'), may hold values from 1 to 16
Outputs:
- input_grad: bfloat16 [131072, 512], P('dom', 'feat')
- self_weight_grad: float32 [512, 512], P('feat')
- neigh_weight_grad: float32 [512, 512], P('feat')
The draws below stay inside these ranges and needn't reach their ends.
Inputs may be any that keep to these rules, and one draw needn't show every extreme that they name: `edge_count`: equals 8192 in at least one partition.
All inputs are finite; a program needn't handle non-finite values.
Results may differ from the reference program's by a relative error of at most 0.0044.
Values may be sent and summed in bfloat16 or wider, within the bound.
No kernel may reach another device: no remote copies, remote signals or barrier semaphores. Data moves between devices by JAX's collectives and lax.ppermute only.
A program may use at most 64 MiB of HBM per device.

```python
import math
import jax
import jax.numpy as jnp
import numpy as np
from jax import lax

D = 512
M_DEV = 1024
SLOT = 32
HUB = 64
E_DEV = 8192
LOCAL = 5120
NV = 131072
NE = 1048576
N_DOM = 128


def draw_edge_count(key, part):
    counts = jax.random.randint(key, (N_DOM,), E_DEV // 4, E_DEV + 1)
    chosen = jax.random.randint(jax.random.fold_in(key, 7), (), 0, N_DOM)
    return counts.at[chosen].set(E_DEV).astype(jnp.int32)


def place_ends(drawn, key, smallest, top_value):
    spot = [jax.random.randint(jax.random.fold_in(key, axis), (), 0, length) for axis, length in enumerate(drawn.shape)]
    main_axis = drawn.shape.index(max(drawn.shape))
    beside = spot[:main_axis] + [(spot[main_axis] + 1) % drawn.shape[main_axis]] + spot[main_axis + 1:]
    return drawn.at[tuple(spot)].set(smallest).at[tuple(beside)].set(top_value)


def shard_levels(stream_key, extent, shards, smallest, largest):
    level = 1.0
    for axis_at, blocks in shards:
        draws = jax.random.uniform(jax.random.fold_in(jax.random.fold_in(stream_key, 6), axis_at), (blocks,), jnp.float32, smallest / len(shards), largest / len(shards))
        level = level * jnp.repeat(jnp.exp(draws), extent[axis_at] // blocks).reshape((-1,) + (1,) * (len(extent) - 1 - axis_at))
    return level


def rank_table(count, skew):
    loads = [(1 << 20) // math.isqrt(grade ** skew) + 1 for grade in range(1, count + 1)]
    deviation = 1 + sum(loads) // (1 << 30)
    return np.cumsum(np.array([max(1, weight // deviation) for weight in loads]))


def ranked(own_key, extent, amount, lean):
    table = rank_table(amount, lean)
    lot = jax.random.randint(jax.random.fold_in(own_key, 1), extent, 0, int(table[amount - 1]))
    standing = jnp.searchsorted(jnp.asarray(table, jnp.int32), lot, side="right")
    return jax.random.permutation(jax.random.fold_in(own_key, 2), amount)[standing].astype(jnp.int32)


def scatter_about(key, extent, deviation, limit, shards=(), kind=jnp.bfloat16):
    entries = deviation * jax.random.normal(key, extent, jnp.float32)
    if shards:
        entries = entries * shard_levels(key, extent, shards, -0.22, 0.18)
    return jnp.clip(entries, -limit, limit).astype(kind)


def setup_inputs(seed: int = 0) -> dict:
    keys = jax.random.split(jax.random.key(seed), 12)
    return {
        "features": scatter_about(keys[0], (NV, D), 1.0, 6.0, ((0, 128), (1, 2))),
        "grad_out": scatter_about(keys[1], (NV, D), 1.0, 6.0, ((0, 128), (1, 2))),
        "pre_act": scatter_about(keys[2], (NV, D), 1.0, 6.0, ((0, 128), (1, 2))),
        "neigh_mean": scatter_about(keys[3], (NV, D), 1.0, 6.0, ((0, 128), (1, 2))),
        "w_self": scatter_about(keys[4], (D, D), D ** -0.5, 0.25, ((0, 2),)),
        "w_neigh": scatter_about(keys[5], (D, D), D ** -0.5, 0.25, ((0, 2),)),
        "edge_from": place_ends(jax.random.randint(keys[6], (NE,), 0, LOCAL), jax.random.fold_in(keys[6], 1), 0, LOCAL - 1).astype(jnp.int32),
        "edge_to": place_ends(ranked(keys[7], (NE,), LOCAL, 2), jax.random.fold_in(keys[7], 3), 0, LOCAL - 1).astype(jnp.int32),
        "edge_count": draw_edge_count(jax.random.fold_in(keys[11], 71), 0),
        "mirror_master": place_ends(jax.random.randint(keys[9], (N_DOM * N_DOM * SLOT,), 0, HUB), jax.random.fold_in(keys[9], 1), 0, HUB - 1).astype(jnp.int32),
        "degrees": place_ends(jax.random.randint(keys[10], (NV,), 1, 17), jax.random.fold_in(keys[10], 1), 1, 16).astype(jnp.int32),
    }


def reference(features, grad_out, pre_act, neigh_mean, w_self, w_neigh, edge_from, edge_to, edge_count, mirror_master, degrees):
    grad_pre = (grad_out.astype(jnp.float32) * (pre_act > 0).astype(jnp.float32)).astype(jnp.bfloat16)
    self_weight_grad = jnp.dot(features.T, grad_pre, preferred_element_type=jnp.float32)
    neigh_weight_grad = jnp.dot(neigh_mean.T, grad_pre, preferred_element_type=jnp.float32)
    self_part = jnp.dot(grad_pre, w_self.T, preferred_element_type=jnp.float32)
    neigh_part = jnp.dot(grad_pre, w_neigh.T, preferred_element_type=jnp.float32)
    scaled = (neigh_part / degrees[:, None].astype(jnp.float32)).astype(jnp.bfloat16)
    mirror_count = N_DOM * SLOT
    local_rows = M_DEV + mirror_count
    owners = jnp.arange(mirror_count, dtype=jnp.int32) // SLOT

    def partition_step(index, totals):
        index = jnp.asarray(index).astype(jnp.int32)
        row_base = (index * M_DEV).astype(jnp.int32)
        masters = lax.dynamic_slice_in_dim(scaled, row_base, M_DEV, 0)
        targets = lax.dynamic_slice_in_dim(mirror_master, (index * mirror_count).astype(jnp.int32), mirror_count, 0)
        global_rows = (owners * M_DEV + targets).astype(jnp.int32)
        tables = jnp.concatenate([masters, scaled[global_rows]], axis=0)
        edge_base = (index * E_DEV).astype(jnp.int32)
        sources = lax.dynamic_slice_in_dim(edge_from, edge_base, E_DEV, 0)
        sinks = lax.dynamic_slice_in_dim(edge_to, edge_base, E_DEV, 0)
        is_live = jnp.arange(E_DEV, dtype=jnp.int32) < edge_count[index]
        contrib = jnp.where(is_live[:, None], tables[sinks].astype(jnp.float32), jnp.float32(0.0))
        summed = jax.ops.segment_sum(contrib, sources, num_segments=local_rows)
        mirror_grad = lax.optimization_barrier(summed[M_DEV:].astype(jnp.bfloat16)).astype(jnp.float32)
        current = lax.dynamic_slice_in_dim(totals, row_base, M_DEV, 0)
        totals = lax.dynamic_update_slice_in_dim(totals, current + summed[:M_DEV], row_base, 0)
        return totals.at[global_rows].add(mirror_grad)

    edge_grad = lax.fori_loop(0, N_DOM, partition_step, jnp.zeros((M_DEV * N_DOM, D), jnp.float32))
    input_grad = (self_part + edge_grad).astype(jnp.bfloat16)
    return input_grad, self_weight_grad, neigh_weight_grad
```

```python
import functools

import jax
import jax.numpy as jnp
from jax import lax
from jax.experimental import pallas as pl
from jax.experimental.pallas import tpu as pltpu
from jax.sharding import PartitionSpec as P

LANES = 128
SUB = 8
CHAINS = 4
UNROLL = 8
VMEM = pl.BlockSpec(memory_space=pltpu.VMEM)
SMEM = pl.BlockSpec(memory_space=pltpu.SMEM)


def picks(asked_ref, group, hub):
    wanted = asked_ref[pl.ds(group, 1), :]
    rows = lax.broadcasted_iota(jnp.int32, (hub, wanted.shape[1]), 0)
    return (rows == wanted).astype(jnp.float32).astype(jnp.bfloat16)


def pack_kernel(slots, asked_ref, hub_ref, pay_ref, out_ref):
    hub = hub_ref.shape[0]
    groups = asked_ref.shape[0]
    per = asked_ref.shape[1] // slots
    pay = out_ref.shape[1] - slots

    def one(group, carry):
        chosen = picks(asked_ref, group, hub)
        rows = lax.dot_general(
            chosen, hub_ref[...], (((0,), (0,)), ((), ())), preferred_element_type=jnp.float32
        ).astype(jnp.bfloat16)
        for k in range(per):
            peer = group * per + k
            out_ref[peer, 0:slots, :] = rows[k * slots : (k + 1) * slots]
            out_ref[peer, slots:, :] = pay_ref[pl.ds(pl.multiple_of(peer * pay, SUB), pay), :]
        return carry

    lax.fori_loop(0, groups, one, 0)


def edge_kernel(slots, from_ref, to_ref, own_ref, got_ref, master_ref, send_ref, table, *sums):
    masters, width = own_ref.shape
    parts = got_ref.shape[0]
    pay = got_ref.shape[1] - slots
    halves = width // LANES
    tall = SUB * halves
    edges = from_ref.shape[0]

    def put(base, block):
        for g in range(block.shape[0] // SUB):
            for h in range(halves):
                at = pl.multiple_of(base + g * tall + h * SUB, SUB)
                table[pl.ds(at, SUB), :] = block[g * SUB : (g + 1) * SUB, h * LANES : (h + 1) * LANES]

    def own(i, carry):
        block = own_ref[pl.ds(pl.multiple_of(i * 32, 32), 32), :].astype(jnp.float32)
        put(i * 32 * halves, block)
        return carry

    lax.fori_loop(0, masters // 32, own, 0)

    def got(p, total):
        put((masters + p * slots) * halves, got_ref[p, 0:slots, :].astype(jnp.float32))
        return total + got_ref[p, slots:, :].astype(jnp.float32)

    total = lax.fori_loop(0, parts, got, jnp.zeros((pay, width), jnp.float32))
    share = total.astype(jnp.bfloat16)

    clear = 16 * SUB

    def zero(i, carry):
        for s in sums:
            s[pl.ds(pl.multiple_of(i * clear, clear), clear), :] = jnp.zeros((clear, LANES), jnp.float32)
        return carry

    lax.fori_loop(0, table.shape[0] // clear, zero, 0)

    step = CHAINS * UNROLL

    def add(i, carry):
        for j in range(step):
            src = from_ref[i * step + j]
            dst = to_ref[i * step + j]
            into = sums[j % CHAINS]
            at = pl.ds(src, halves, stride=SUB)
            into[at, :] = into[at, :] + table[pl.ds(dst, halves, stride=SUB), :]
        return carry

    lax.fori_loop(0, edges // step, add, 0)

    def merged(base, rows, h):
        tiles = []
        for g in range(rows // SUB):
            at = pl.ds(pl.multiple_of(base + g * tall + h * SUB, SUB), SUB)
            value = sums[0][at, :]
            for s in sums[1:]:
                value = value + s[at, :]
            tiles.append(value)
        return jnp.concatenate(tiles, axis=0)

    def finish(i, carry):
        for h in range(halves):
            cols = slice(h * LANES, (h + 1) * LANES)
            master_ref[pl.ds(pl.multiple_of(i * 32, 32), 32), cols] = merged(i * 32 * halves, 32, h)
        return carry

    lax.fori_loop(0, masters // 32, finish, 0)

    def reply(p, carry):
        for h in range(halves):
            cols = slice(h * LANES, (h + 1) * LANES)
            block = merged((masters + p * slots) * halves, slots, h)
            send_ref[p, 0:slots, cols] = block.astype(jnp.bfloat16)
        send_ref[p, slots:, :] = share
        return carry

    lax.fori_loop(0, parts, reply, 0)


def final_kernel(slots, hub, asked_ref, got_ref, pre_ref, grad_ref, self_ref, neigh_ref):
    groups = asked_ref.shape[0]
    per = asked_ref.shape[1] // slots
    parts = got_ref.shape[0]
    pay = got_ref.shape[1] - slots
    width = pre_ref.shape[1]

    def one(group, total):
        chosen = picks(asked_ref, group, hub)
        rows = jnp.concatenate([got_ref[group * per + k, 0:slots, :] for k in range(per)], axis=0)
        return total + jnp.dot(chosen, rows, preferred_element_type=jnp.float32)

    total = lax.fori_loop(0, groups, one, jnp.zeros((hub, width), jnp.float32))
    grad_ref[0:hub, :] = (pre_ref[0:hub, :] + total).astype(jnp.bfloat16)
    grad_ref[hub:, :] = pre_ref[hub:, :].astype(jnp.bfloat16)

    quarter = parts // 4
    for which, ref in ((0, self_ref), (1, neigh_ref)):
        for half in range(2):

            def place(i, carry, which=which, ref=ref, half=half):
                peer = (which * 2 + half) * quarter + i
                rows = pl.ds(pl.multiple_of(i * pay, SUB), pay)
                ref[rows, half * width : (half + 1) * width] = got_ref[peer, slots:, :].astype(jnp.float32)
                return carry

            lax.fori_loop(0, quarter, place, 0)


def on_device(
    features,
    grad_out,
    pre_act,
    neigh_mean,
    w_self,
    w_neigh,
    edge_from,
    edge_to,
    edge_count,
    mirror_master,
    degrees,
):
    masters, width = features.shape
    parts = lax.axis_size("dom")
    mirrors = mirror_master.shape[0]
    slots = mirrors // parts
    hub = min(masters, 64)
    local = masters + mirrors
    halves = width // LANES
    edges = edge_from.shape[0]

    wanted = mirror_master.reshape(parts, slots)
    asked = lax.all_to_all(wanted, "dom", split_axis=0, concat_axis=0, tiled=True)
    asked = asked.reshape(mirrors // LANES, LANES)

    def spot(row):
        return (row // SUB) * (SUB * halves) + row % SUB

    live = jnp.arange(edges, dtype=jnp.int32) < edge_count[0]
    from_at = spot(jnp.where(live, edge_from, local))
    to_at = spot(edge_to)

    grad_pre = (grad_out.astype(jnp.float32) * (pre_act > 0).astype(jnp.float32)).astype(jnp.bfloat16)
    other = lax.ppermute(grad_pre, "feat", [(0, 1), (1, 0)])
    first = lax.axis_index("feat") == 0
    block_cols = jnp.concatenate(
        [jnp.where(first, grad_pre, other), jnp.where(first, other, grad_pre)], axis=1
    )
    contract = (((1,), (1,)), ((), ()))
    over_rows = (((0,), (0,)), ((), ()))
    neigh_part = lax.dot_general(block_cols, w_neigh, contract, preferred_element_type=jnp.float32)
    scaled = (neigh_part / degrees[:, None].astype(jnp.float32)).astype(jnp.bfloat16)
    grad_self = lax.dot_general(features, block_cols, over_rows, preferred_element_type=jnp.float32)
    grad_neigh = lax.dot_general(neigh_mean, block_cols, over_rows, preferred_element_type=jnp.float32)
    pay = jnp.concatenate(
        [grad_self[:, :width], grad_self[:, width:], grad_neigh[:, :width], grad_neigh[:, width:]], axis=0
    ).astype(jnp.bfloat16)
    tail = pay.shape[0] // parts

    message = jax.ShapeDtypeStruct((parts, slots + tail, width), jnp.bfloat16)
    sent = pl.pallas_call(
        functools.partial(pack_kernel, slots),
        out_shape=message,
        in_specs=[VMEM] * 3,
        out_specs=VMEM,
        name="pack",
    )(asked, scaled[:hub], pay)
    got = lax.all_to_all(sent, "dom", split_axis=0, concat_axis=0, tiled=True)

    lanes = local * halves
    spare = SUB * halves
    master_sum, back = pl.pallas_call(
        functools.partial(edge_kernel, slots),
        out_shape=(jax.ShapeDtypeStruct((masters, width), jnp.float32), message),
        in_specs=[SMEM, SMEM, VMEM, VMEM],
        out_specs=[VMEM, VMEM],
        scratch_shapes=[pltpu.VMEM((lanes, LANES), jnp.float32)]
        + [pltpu.VMEM((lanes + spare, LANES), jnp.float32) for _ in range(CHAINS)],
        name="edges",
    )(from_at, to_at, scaled, got)
    home = lax.all_to_all(back, "dom", split_axis=0, concat_axis=0, tiled=True)

    self_part = lax.dot_general(block_cols, w_self, contract, preferred_element_type=jnp.float32)
    pre = self_part + master_sum
    return pl.pallas_call(
        functools.partial(final_kernel, slots, hub),
        out_shape=(
            jax.ShapeDtypeStruct((masters, width), jnp.bfloat16),
            jax.ShapeDtypeStruct(w_self.shape, jnp.float32),
            jax.ShapeDtypeStruct(w_neigh.shape, jnp.float32),
        ),
        in_specs=[VMEM] * 3,
        out_specs=[VMEM] * 3,
        name="final",
    )(asked, home, pre)


def solution(mesh):
    placed = (
        P("dom", "feat"),
        P("dom", "feat"),
        P("dom", "feat"),
        P("dom", "feat"),
        P("feat", None),
        P("feat", None),
        P("dom"),
        P("dom"),
        P("dom"),
        P("dom"),
        P("dom"),
    )
    return jax.shard_map(
        on_device,
        mesh=mesh,
        in_specs=placed,
        out_specs=(P("dom", "feat"), P("feat", None), P("feat", None)),
        check_vma=False,
    )
```

```python
import functools

import jax
import jax.numpy as jnp
from jax import lax
from jax.experimental import pallas as pl
from jax.experimental.pallas import tpu as pltpu
from jax.sharding import PartitionSpec as P

LANES = 128
SUB = 8
CHAINS = 4
UNROLL = 8
VMEM = pl.BlockSpec(memory_space=pltpu.VMEM)
SMEM = pl.BlockSpec(memory_space=pltpu.SMEM)


def near(array):
    return pltpu.with_memory_space_constraint(array, pltpu.VMEM)


def picks(wanted, hub):
    rows = lax.broadcasted_iota(jnp.int32, (hub, wanted.shape[1]), 0)
    return (rows == wanted).astype(jnp.float32).astype(jnp.bfloat16)


def grouped(asked_ref, slots):
    per = LANES // slots
    rows = asked_ref.shape[0] // per
    lane = lax.broadcasted_iota(jnp.int32, (rows, LANES), 1)
    dense = asked_ref[pl.ds(0, rows, stride=per), :]
    for k in range(1, per):
        part = pltpu.roll(asked_ref[pl.ds(k, rows, stride=per), :], k * slots, 1)
        dense = jnp.where(lane < k * slots, dense, part)
    return dense


def pack_kernel(slots, asked_ref, hub_ref, pay_ref, out_ref, dense_ref):
    hub, width = hub_ref.shape
    parts = out_ref.shape[0]
    pay = out_ref.shape[1] - slots
    dense_ref[...] = grouped(asked_ref, slots)
    rows = min(4, dense_ref.shape[0])
    peers = rows * LANES // slots

    def one(i, carry):
        for r in range(rows):
            chosen = picks(dense_ref[pl.ds(i * rows + r, 1), :], hub)
            found = lax.dot_general(
                chosen, hub_ref[...], (((0,), (0,)), ((), ())), preferred_element_type=jnp.float32
            ).astype(jnp.bfloat16)
            for k in range(LANES // slots):
                peer = i * peers + r * (LANES // slots) + k
                out_ref[peer, 0:slots, :] = found[k * slots : (k + 1) * slots]
                out_ref[peer, slots:, :] = pay_ref[pl.ds(pl.multiple_of(peer * pay, SUB), pay), :]
        return carry

    lax.fori_loop(0, parts // peers, one, 0)


def edge_kernel(slots, from_ref, to_ref, own_ref, got_ref, self_ref, pre_ref, send_ref, table, *sums):
    masters, width = own_ref.shape
    parts = got_ref.shape[0]
    pay = got_ref.shape[1] - slots
    halves = width // LANES
    tall = SUB * halves
    edges = from_ref.shape[0]

    def put(base, block):
        for g in range(block.shape[0] // SUB):
            for h in range(halves):
                at = pl.multiple_of(base + g * tall + h * SUB, SUB)
                table[pl.ds(at, SUB), :] = block[g * SUB : (g + 1) * SUB, h * LANES : (h + 1) * LANES]

    def own(i, carry):
        block = own_ref[pl.ds(pl.multiple_of(i * 32, 32), 32), :].astype(jnp.float32)
        put(i * 32 * halves, block)
        return carry

    lax.fori_loop(0, masters // 32, own, 0)

    def got(p, total):
        put((masters + p * slots) * halves, got_ref[p, 0:slots, :].astype(jnp.float32))
        return total + got_ref[p, slots:, :].astype(jnp.float32)

    total = lax.fori_loop(0, parts, got, jnp.zeros((pay, width), jnp.float32))
    share = total.astype(jnp.bfloat16)

    clear = 16 * SUB

    def zero(i, carry):
        for s in sums:
            s[pl.ds(pl.multiple_of(i * clear, clear), clear), :] = jnp.zeros((clear, LANES), jnp.float32)
        return carry

    lax.fori_loop(0, table.shape[0] // clear, zero, 0)

    step = CHAINS * UNROLL

    def add(i, carry):
        for j in range(step):
            src = from_ref[i * step + j]
            dst = to_ref[i * step + j]
            into = sums[j % CHAINS]
            at = pl.ds(src, halves, stride=SUB)
            into[at, :] = into[at, :] + table[pl.ds(dst, halves, stride=SUB), :]
        return carry

    lax.fori_loop(0, edges // step, add, 0)

    def merged(base, rows, h):
        tiles = []
        for g in range(rows // SUB):
            at = pl.ds(pl.multiple_of(base + g * tall + h * SUB, SUB), SUB)
            value = sums[0][at, :]
            for s in sums[1:]:
                value = value + s[at, :]
            tiles.append(value)
        return jnp.concatenate(tiles, axis=0)

    def finish(i, carry):
        for h in range(halves):
            rows = pl.ds(pl.multiple_of(i * 32, 32), 32)
            cols = slice(h * LANES, (h + 1) * LANES)
            pre_ref[rows, cols] = self_ref[rows, cols] + merged(i * 32 * halves, 32, h)
        return carry

    lax.fori_loop(0, masters // 32, finish, 0)

    def reply(p, carry):
        for h in range(halves):
            cols = slice(h * LANES, (h + 1) * LANES)
            block = merged((masters + p * slots) * halves, slots, h)
            send_ref[p, 0:slots, cols] = block.astype(jnp.bfloat16)
        send_ref[p, slots:, :] = share
        return carry

    lax.fori_loop(0, parts, reply, 0)


def final_kernel(slots, hub, dense_ref, got_ref, pre_ref, grad_ref, self_ref, neigh_ref):
    parts = got_ref.shape[0]
    pay = got_ref.shape[1] - slots
    width = pre_ref.shape[1]
    rows = min(4, dense_ref.shape[0])
    peers = rows * LANES // slots

    def one(i, total):
        chosen = [picks(dense_ref[pl.ds(i * rows + r, 1), :], hub) for r in range(rows)]
        found = [got_ref[i * peers + k, 0:slots, :] for k in range(peers)]
        return total + jnp.dot(
            jnp.concatenate(chosen, axis=1),
            jnp.concatenate(found, axis=0),
            preferred_element_type=jnp.float32,
        )

    total = lax.fori_loop(0, parts // peers, one, jnp.zeros((hub, width), jnp.float32))
    grad_ref[0:hub, :] = (pre_ref[0:hub, :] + total).astype(jnp.bfloat16)
    grad_ref[hub:, :] = pre_ref[hub:, :].astype(jnp.bfloat16)

    quarter = parts // 4
    for which, ref in ((0, self_ref), (1, neigh_ref)):
        for half in range(2):

            def place(i, carry, which=which, ref=ref, half=half):
                peer = (which * 2 + half) * quarter + i
                rows = pl.ds(pl.multiple_of(i * pay, SUB), pay)
                ref[rows, half * width : (half + 1) * width] = got_ref[peer, slots:, :].astype(jnp.float32)
                return carry

            lax.fori_loop(0, quarter, place, 0)


def on_device(
    features,
    grad_out,
    pre_act,
    neigh_mean,
    w_self,
    w_neigh,
    edge_from,
    edge_to,
    edge_count,
    mirror_master,
    degrees,
):
    masters, width = features.shape
    parts = lax.axis_size("dom")
    mirrors = mirror_master.shape[0]
    slots = mirrors // parts
    hub = min(masters, 64)
    local = masters + mirrors
    halves = width // LANES
    edges = edge_from.shape[0]

    wanted = jnp.pad(mirror_master.reshape(parts, slots), ((0, 0), (0, LANES - slots)))
    asked = lax.all_to_all(wanted, "dom", split_axis=0, concat_axis=0, tiled=True)

    def spot(row):
        return (row // SUB) * (SUB * halves) + row % SUB

    live = jnp.arange(edges, dtype=jnp.int32) < edge_count[0]
    from_at = spot(jnp.where(live, edge_from, local))
    to_at = spot(edge_to)

    grad_pre = (grad_out.astype(jnp.float32) * (pre_act > 0).astype(jnp.float32)).astype(jnp.bfloat16)
    other = lax.ppermute(grad_pre, "feat", [(0, 1), (1, 0)])
    first = lax.axis_index("feat") == 0
    block_cols = jnp.concatenate(
        [jnp.where(first, grad_pre, other), jnp.where(first, other, grad_pre)], axis=1
    )
    contract = (((1,), (1,)), ((), ()))
    over_rows = (((0,), (0,)), ((), ()))
    neigh_part = lax.dot_general(block_cols, w_neigh, contract, preferred_element_type=jnp.float32)
    scaled = (neigh_part / degrees[:, None].astype(jnp.float32)).astype(jnp.bfloat16)
    self_part = lax.dot_general(block_cols, w_self, contract, preferred_element_type=jnp.float32)
    grad_self = lax.dot_general(features, block_cols, over_rows, preferred_element_type=jnp.float32)
    grad_neigh = lax.dot_general(neigh_mean, block_cols, over_rows, preferred_element_type=jnp.float32)
    pay = jnp.concatenate(
        [grad_self[:, :width], grad_self[:, width:], grad_neigh[:, :width], grad_neigh[:, width:]], axis=0
    ).astype(jnp.bfloat16)
    tail = pay.shape[0] // parts

    message = pltpu.VMEM((parts, slots + tail, width), jnp.bfloat16)
    sent, dense = pl.pallas_call(
        functools.partial(pack_kernel, slots),
        out_shape=(message, jax.ShapeDtypeStruct((mirrors // LANES, LANES), jnp.int32)),
        in_specs=[VMEM] * 3,
        out_specs=[VMEM] * 2,
        compiler_params=pltpu.CompilerParams(vmem_limit_bytes=8 << 20),
        name="pack",
    )(asked, near(scaled[:hub]), near(pay))
    sent, from_at, to_at, self_part, scaled, dense = lax.optimization_barrier(
        (sent, from_at, to_at, self_part, scaled, dense)
    )
    got = lax.all_to_all(sent, "dom", split_axis=0, concat_axis=0, tiled=True)

    lanes = local * halves
    spare = SUB * halves
    pre, back = pl.pallas_call(
        functools.partial(edge_kernel, slots),
        out_shape=(pltpu.VMEM((masters, width), jnp.float32), message),
        in_specs=[SMEM, SMEM, VMEM, VMEM, VMEM],
        out_specs=[VMEM, VMEM],
        scratch_shapes=[pltpu.VMEM((lanes, LANES), jnp.float32)]
        + [pltpu.VMEM((lanes + spare, LANES), jnp.float32) for _ in range(CHAINS)],
        compiler_params=pltpu.CompilerParams(vmem_limit_bytes=36 << 20),
        name="edges",
    )(from_at, to_at, near(scaled), near(got), near(self_part))
    home = lax.all_to_all(back, "dom", split_axis=0, concat_axis=0, tiled=True)

    return pl.pallas_call(
        functools.partial(final_kernel, slots, hub),
        out_shape=(
            jax.ShapeDtypeStruct((masters, width), jnp.bfloat16),
            jax.ShapeDtypeStruct(w_self.shape, jnp.float32),
            jax.ShapeDtypeStruct(w_neigh.shape, jnp.float32),
        ),
        in_specs=[VMEM] * 3,
        out_specs=[VMEM] * 3,
        compiler_params=pltpu.CompilerParams(vmem_limit_bytes=12 << 20),
        name="final",
    )(dense, near(home), near(pre))


def solution(mesh):
    placed = (
        P("dom", "feat"),
        P("dom", "feat"),
        P("dom", "feat"),
        P("dom", "feat"),
        P("feat", None),
        P("feat", None),
        P("dom"),
        P("dom"),
        P("dom"),
        P("dom"),
        P("dom"),
    )
    return jax.shard_map(
        on_device,
        mesh=mesh,
        in_specs=placed,
        out_specs=(P("dom", "feat"), P("feat", None), P("feat", None)),
        check_vma=False,
    )
```

```python
import functools

import jax
import jax.numpy as jnp
from jax import lax
from jax.experimental import pallas as pl
from jax.experimental.pallas import tpu as pltpu
from jax.sharding import PartitionSpec as P

LANES = 128
SUB = 8
GRID = (4, 8, 4)
CHAINS = 4
UNROLL = 8
VMEM = pl.BlockSpec(memory_space=pltpu.VMEM)
SMEM = pl.BlockSpec(memory_space=pltpu.SMEM)


def near(array):
    return pltpu.with_memory_space_constraint(array, pltpu.VMEM)


def ring(axis, shift):
    nx, nz, ny = GRID
    pairs = []
    for x in range(nx):
        for z in range(nz):
            for y in range(ny):
                tx = (x + shift) % nx if axis == "x" else x
                ty = (y + shift) % ny if axis == "y" else y
                pairs.append(((x * nz + z) * ny + y, (tx * nz + z) * ny + ty))
    return pairs


def columns():
    nx, nz, ny = GRID
    return [[(x * nz + z) * ny + y for z in range(nz)] for x in range(nx) for y in range(ny)]


def sum_of(arrays):
    total = arrays[0].astype(jnp.float32)
    for a in arrays[1:]:
        total = total + a.astype(jnp.float32)
    return total


def picks_kernel(spot_ref, out_ref):
    groups, lanes = spot_ref.shape
    rows = out_ref.shape[2]

    def one(g, carry):
        spread = jnp.broadcast_to(spot_ref[pl.ds(g, 1), :].astype(jnp.float32), (LANES, lanes))
        across = jnp.concatenate([jnp.transpose(spread)] * (rows // min(rows, LANES)), axis=1)
        hub = lax.broadcasted_iota(jnp.int32, (lanes, across.shape[1]), 1).astype(jnp.float32)
        chosen = (across == hub).astype(jnp.float32).astype(jnp.bfloat16)
        out_ref[g] = chosen[:, 0:rows]
        return carry

    lax.fori_loop(0, groups, one, 0)


def edge_kernel(grid, slots, from_ref, to_ref, place_ref, own_ref, self_ref, spot_ref, pick_ref, *rest):
    nx, nz, ny = grid
    got_x = rest[0:ny]
    got_y = rest[ny : ny + nx]
    pre_ref = rest[ny + nx]
    back_x = rest[ny + nx + 1 : 2 * ny + nx + 1]
    back_y = rest[2 * ny + nx + 1 : 2 * (ny + nx) + 1]
    table = rest[2 * (ny + nx) + 1]
    sums = rest[2 * (ny + nx) + 2 :]
    masters, width = own_ref.shape
    halves = width // LANES
    tall = SUB * halves
    edges = from_ref.shape[0]
    deep = nz // 2

    def put(base, block):
        for g in range(block.shape[0] // SUB):
            for h in range(halves):
                at = pl.multiple_of(base + g * tall + h * SUB, SUB)
                table[pl.ds(at, SUB), :] = block[g * SUB : (g + 1) * SUB, h * LANES : (h + 1) * LANES]

    def own(i, carry):
        put(i * 32 * halves, own_ref[pl.ds(pl.multiple_of(i * 32, 32), 32), :].astype(jnp.float32))
        return carry

    lax.fori_loop(0, masters // 32, own, 0)

    def base_of(x, y, high, z):
        owner = (x * nz + high * deep + z) * ny + y
        return (masters + owner * slots) * halves

    def blocks(high, first, second):
        if high:
            x, y = place_ref[first], place_ref[nx + second]
        else:
            x, y = place_ref[second], place_ref[nx + first]
        return x, y, (x * ny + y) * 2 + high

    for high, got in ((0, got_x), (1, got_y)):
        for first in range(len(got)):

            def fetch(second, carry, high=high, first=first, got=got):
                x, y, group = blocks(high, first, second)
                rows = jnp.dot(pick_ref[group], got[first][second], preferred_element_type=jnp.float32)
                for z in range(deep):
                    put(base_of(x, y, high, z), rows[z * slots : (z + 1) * slots])
                return carry

            for second in range(got[first].shape[0]):
                fetch(second, 0)

    clear = 16 * SUB

    def zero(i, carry):
        for s in sums:
            s[pl.ds(pl.multiple_of(i * clear, clear), clear), :] = jnp.zeros((clear, LANES), jnp.float32)
        return carry

    lax.fori_loop(0, table.shape[0] // clear, zero, 0)

    step = CHAINS * UNROLL

    def add(i, carry):
        for j in range(step):
            src = from_ref[i * step + j]
            dst = to_ref[i * step + j]
            into = sums[j % CHAINS]
            at = pl.ds(src, halves, stride=SUB)
            into[at, :] = into[at, :] + table[pl.ds(dst, halves, stride=SUB), :]
        return carry

    lax.fori_loop(0, edges // step, add, 0)

    def merged(base, rows, h):
        tiles = []
        for g in range(rows // SUB):
            at = pl.ds(pl.multiple_of(base + g * tall + h * SUB, SUB), SUB)
            value = sums[0][at, :]
            for s in sums[1:]:
                value = value + s[at, :]
            tiles.append(value)
        return jnp.concatenate(tiles, axis=0)

    def finish(i, carry):
        for h in range(halves):
            rows = pl.ds(pl.multiple_of(i * 32, 32), 32)
            cols = slice(h * LANES, (h + 1) * LANES)
            pre_ref[rows, cols] = self_ref[rows, cols] + merged(i * 32 * halves, 32, h)
        return carry

    lax.fori_loop(0, masters // 32, finish, 0)

    for high, back in ((0, back_x), (1, back_y)):
        for first in range(len(back)):
            for second in range(back[first].shape[0]):
                x, y, group = blocks(high, first, second)
                target = spot_ref[pl.ds(group, 1), :]
                rows = lax.broadcasted_iota(jnp.int32, (back[first].shape[1], target.shape[1]), 0)
                chosen = (rows == target).astype(jnp.float32).astype(jnp.bfloat16)
                block = jnp.concatenate(
                    [
                        jnp.concatenate(
                            [merged(base_of(x, y, high, z), slots, h) for h in range(halves)], axis=1
                        ).astype(jnp.bfloat16)
                        for z in range(deep)
                    ],
                    axis=0,
                )
                back[first][second] = jnp.dot(
                    chosen, block, preferred_element_type=jnp.float32
                ).astype(jnp.bfloat16)


def final_kernel(home_ref, pre_ref, weight_ref, grad_ref, self_ref, neigh_ref):
    hub = home_ref.shape[1]
    parts, pay, width = weight_ref.shape
    total = pre_ref[0:hub, :]
    for z in range(home_ref.shape[0]):
        total = total + home_ref[z].astype(jnp.float32)
    grad_ref[0:hub, :] = total.astype(jnp.bfloat16)
    grad_ref[hub:, :] = pre_ref[hub:, :].astype(jnp.bfloat16)
    quarter = parts // 4
    for which, ref in ((0, self_ref), (1, neigh_ref)):
        for half in range(2):

            def place(i, carry, which=which, ref=ref, half=half):
                peer = (which * 2 + half) * quarter + i
                rows = pl.ds(pl.multiple_of(i * pay, SUB), pay)
                ref[rows, half * width : (half + 1) * width] = weight_ref[peer].astype(jnp.float32)
                return carry

            lax.fori_loop(0, quarter, place, 0)


def on_device(
    features,
    grad_out,
    pre_act,
    neigh_mean,
    w_self,
    w_neigh,
    edge_from,
    edge_to,
    edge_count,
    mirror_master,
    degrees,
):
    nx, nz, ny = GRID
    deep = nz // 2
    masters, width = features.shape
    parts = lax.axis_size("dom")
    mirrors = mirror_master.shape[0]
    slots = mirrors // parts
    hub = min(masters, 64)
    local = masters + mirrors
    halves = width // LANES
    edges = edge_from.shape[0]
    contract = (((1,), (1,)), ((), ()))
    over_rows = (((0,), (0,)), ((), ()))
    first = lax.axis_index("feat") == 0

    def both(rows_out, rows_act):
        mine = (rows_out.astype(jnp.float32) * (rows_act > 0).astype(jnp.float32)).astype(jnp.bfloat16)
        other = lax.ppermute(mine, "feat", [(0, 1), (1, 0)])
        return jnp.concatenate([jnp.where(first, mine, other), jnp.where(first, other, mine)], axis=1)

    def scale(cols, degree):
        part = lax.dot_general(cols, w_neigh, contract, preferred_element_type=jnp.float32)
        return (part / degree[:, None].astype(jnp.float32)).astype(jnp.bfloat16)

    shared = scale(both(grad_out[:hub], pre_act[:hub]), degrees[:hub])
    column = lax.all_to_all(
        jnp.broadcast_to(shared, (nz, *shared.shape)),
        "dom",
        split_axis=0,
        concat_axis=0,
        axis_index_groups=columns(),
        tiled=True,
    )
    column, grad_out, pre_act = lax.optimization_barrier((column, grad_out, pre_act))

    low = column[:deep].reshape(deep * hub, width)
    high = column[deep:].reshape(deep * hub, width)
    low_set = jnp.stack([low] + [lax.ppermute(low, "dom", ring("x", k)) for k in range(1, nx)])
    high_set = jnp.stack([high] + [lax.ppermute(high, "dom", ring("y", k)) for k in range(1, ny)])

    block_cols = both(grad_out, pre_act)
    scaled = scale(block_cols, degrees)
    self_part = lax.dot_general(block_cols, w_self, contract, preferred_element_type=jnp.float32)
    grad_self = lax.dot_general(features, block_cols, over_rows, preferred_element_type=jnp.float32)
    grad_neigh = lax.dot_general(neigh_mean, block_cols, over_rows, preferred_element_type=jnp.float32)
    pay = jnp.concatenate(
        [grad_self[:, :width], grad_self[:, width:], grad_neigh[:, :width], grad_neigh[:, width:]], axis=0
    ).astype(jnp.bfloat16)
    tail = pay.shape[0] // parts

    low_set, high_set, pay = lax.optimization_barrier((low_set, high_set, pay))
    low_got = [low_set] + [lax.ppermute(low_set, "dom", ring("y", k)) for k in range(1, ny)]
    high_got = [high_set] + [lax.ppermute(high_set, "dom", ring("x", k)) for k in range(1, nx)]
    pieces = lax.all_to_all(
        pay.reshape(parts, tail, width), "dom", split_axis=0, concat_axis=0, tiled=True
    )

    order = mirror_master.reshape(nx, 2, deep, ny, slots).transpose(0, 3, 1, 2, 4)
    spots = order.reshape(nx * ny * 2, deep * slots) + jnp.repeat(
        jnp.arange(deep, dtype=jnp.int32) * hub, slots
    )
    chosen = pl.pallas_call(
        picks_kernel,
        out_shape=pltpu.VMEM((nx * ny * 2, deep * slots, deep * hub), jnp.bfloat16),
        in_specs=[VMEM],
        out_specs=VMEM,
        compiler_params=pltpu.CompilerParams(vmem_limit_bytes=8 << 20),
        name="picks",
    )(spots)

    def spot(row):
        return (row // SUB) * (SUB * halves) + row % SUB

    live = jnp.arange(edges, dtype=jnp.int32) < edge_count[0]
    from_at = spot(jnp.where(live, edge_from, local))
    to_at = spot(edge_to)
    me = lax.axis_index("dom")
    my_x, my_y = me // (nz * ny), me % ny
    place = jnp.concatenate(
        [(my_x - jnp.arange(nx, dtype=jnp.int32)) % nx, (my_y - jnp.arange(ny, dtype=jnp.int32)) % ny]
    ).astype(jnp.int32)

    lanes = local * halves
    low_type = jax.ShapeDtypeStruct(low_set.shape, jnp.bfloat16)
    high_type = jax.ShapeDtypeStruct(high_set.shape, jnp.bfloat16)
    results = pl.pallas_call(
        functools.partial(edge_kernel, GRID, slots),
        out_shape=[jax.ShapeDtypeStruct((masters, width), jnp.float32)] + [low_type] * ny + [high_type] * nx,
        in_specs=[SMEM] * 3 + [VMEM] * (4 + nx + ny),
        out_specs=[VMEM] * (1 + nx + ny),
        scratch_shapes=[pltpu.VMEM((lanes, LANES), jnp.float32)]
        + [pltpu.VMEM((lanes + SUB * halves, LANES), jnp.float32) for _ in range(CHAINS)],
        compiler_params=pltpu.CompilerParams(vmem_limit_bytes=34 << 20),
        name="edges",
    )(from_at, to_at, place, *(near(a) for a in (scaled, self_part, spots, chosen, *low_got, *high_got)))
    pre, low_back, high_back = results[0], results[1 : 1 + ny], results[1 + ny :]

    share = jnp.sum(pieces.astype(jnp.float32), axis=0).astype(jnp.bfloat16)
    low_back, high_back, share = lax.optimization_barrier((low_back, high_back, share))
    low_part = [low_back[0]] + [lax.ppermute(low_back[k], "dom", ring("y", -k)) for k in range(1, ny)]
    high_part = [high_back[0]] + [lax.ppermute(high_back[k], "dom", ring("x", -k)) for k in range(1, nx)]
    weights = lax.all_to_all(
        jnp.broadcast_to(share, (parts, *share.shape)), "dom", split_axis=0, concat_axis=0, tiled=True
    )
    low_sum = [sum_of([p[k] for p in low_part]) for k in range(nx)]
    high_sum = [sum_of([p[k] for p in high_part]) for k in range(ny)]
    low_sent = [low_sum[0]] + [
        lax.ppermute(low_sum[k].astype(jnp.bfloat16), "dom", ring("x", -k)) for k in range(1, nx)
    ]
    high_sent = [high_sum[0]] + [
        lax.ppermute(high_sum[k].astype(jnp.bfloat16), "dom", ring("y", -k)) for k in range(1, ny)
    ]
    column_sum = jnp.concatenate([sum_of(low_sent), sum_of(high_sent)], axis=0).astype(jnp.bfloat16)
    column_sum, weights, pre = lax.optimization_barrier((column_sum, weights, pre))
    home = lax.all_to_all(
        column_sum.reshape(nz, hub, width),
        "dom",
        split_axis=0,
        concat_axis=0,
        axis_index_groups=columns(),
        tiled=True,
    )
    return pl.pallas_call(
        final_kernel,
        out_shape=(
            jax.ShapeDtypeStruct((masters, width), jnp.bfloat16),
            jax.ShapeDtypeStruct(w_self.shape, jnp.float32),
            jax.ShapeDtypeStruct(w_neigh.shape, jnp.float32),
        ),
        in_specs=[VMEM] * 3,
        out_specs=[VMEM] * 3,
        compiler_params=pltpu.CompilerParams(vmem_limit_bytes=12 << 20),
        name="final",
    )(near(home), near(pre), near(weights))


def solution(mesh):
    placed = (
        P("dom", "feat"),
        P("dom", "feat"),
        P("dom", "feat"),
        P("dom", "feat"),
        P("feat", None),
        P("feat", None),
        P("dom"),
        P("dom"),
        P("dom"),
        P("dom"),
        P("dom"),
    )

    return jax.shard_map(
        on_device,
        mesh=mesh,
        in_specs=placed,
        out_specs=(P("dom", "feat"), P("feat", None), P("feat", None)),
        check_vma=False,
    )
```

```python
import functools

import jax
import jax.numpy as jnp
from jax import lax
from jax.experimental import pallas as pl
from jax.experimental.pallas import tpu as pltpu
from jax.sharding import PartitionSpec as P

LANES = 128
SUB = 8
GRID = (4, 8, 4)
CHAINS = 4
UNROLL = 8
VMEM = pl.BlockSpec(memory_space=pltpu.VMEM)
SMEM = pl.BlockSpec(memory_space=pltpu.SMEM)


def near(array):
    return pltpu.with_memory_space_constraint(array, pltpu.VMEM)


def ring(axis, shift):
    nx, nz, ny = GRID
    pairs = []
    for x in range(nx):
        for z in range(nz):
            for y in range(ny):
                tx = (x + shift) % nx if axis == "x" else x
                ty = (y + shift) % ny if axis == "y" else y
                pairs.append(((x * nz + z) * ny + y, (tx * nz + z) * ny + ty))
    return pairs


def columns():
    nx, nz, ny = GRID
    return [[(x * nz + z) * ny + y for z in range(nz)] for x in range(nx) for y in range(ny)]


def sum_of(arrays):
    total = arrays[0].astype(jnp.float32)
    for a in arrays[1:]:
        total = total + a.astype(jnp.float32)
    return total


def picks_kernel(spot_ref, out_ref):
    groups, lanes = spot_ref.shape
    rows = out_ref.shape[2]

    def one(g, carry):
        spread = jnp.broadcast_to(spot_ref[pl.ds(g, 1), :].astype(jnp.float32), (LANES, lanes))
        across = jnp.concatenate([jnp.transpose(spread)] * (rows // min(rows, LANES)), axis=1)
        hub = lax.broadcasted_iota(jnp.int32, (lanes, across.shape[1]), 1).astype(jnp.float32)
        chosen = (across == hub).astype(jnp.float32).astype(jnp.bfloat16)
        out_ref[g] = chosen[:, 0:rows]
        return carry

    lax.fori_loop(0, groups, one, 0)


def edge_kernel(grid, slots, from_ref, to_ref, place_ref, own_ref, self_ref, spot_ref, pick_ref, *rest):
    nx, nz, ny = grid
    got_x = rest[0:ny]
    got_y = rest[ny : ny + nx]
    pre_ref = rest[ny + nx]
    back_x = rest[ny + nx + 1 : 2 * ny + nx + 1]
    back_y = rest[2 * ny + nx + 1 : 2 * (ny + nx) + 1]
    table = rest[2 * (ny + nx) + 1]
    sums = rest[2 * (ny + nx) + 2 :]
    masters, width = own_ref.shape
    halves = width // LANES
    tall = SUB * halves
    edges = from_ref.shape[0]
    deep = nz // 2

    def put(base, block):
        for g in range(block.shape[0] // SUB):
            for h in range(halves):
                at = pl.multiple_of(base + g * tall + h * SUB, SUB)
                table[pl.ds(at, SUB), :] = block[g * SUB : (g + 1) * SUB, h * LANES : (h + 1) * LANES]

    def own(i, carry):
        put(i * 32 * halves, own_ref[pl.ds(pl.multiple_of(i * 32, 32), 32), :].astype(jnp.float32))
        return carry

    lax.fori_loop(0, masters // 32, own, 0)

    def base_of(x, y, high, z):
        owner = (x * nz + high * deep + z) * ny + y
        return (masters + owner * slots) * halves

    def blocks(high, first, second):
        if high:
            x, y = place_ref[first], place_ref[nx + second]
        else:
            x, y = place_ref[second], place_ref[nx + first]
        return x, y, (x * ny + y) * 2 + high

    for high, got in ((0, got_x), (1, got_y)):
        for first in range(len(got)):

            def fetch(second, carry, high=high, first=first, got=got):
                x, y, group = blocks(high, first, second)
                rows = jnp.dot(pick_ref[group], got[first][second], preferred_element_type=jnp.float32)
                for z in range(deep):
                    put(base_of(x, y, high, z), rows[z * slots : (z + 1) * slots])
                return carry

            for second in range(got[first].shape[0]):
                fetch(second, 0)

    clear = 16 * SUB

    def zero(i, carry):
        for s in sums:
            s[pl.ds(pl.multiple_of(i * clear, clear), clear), :] = jnp.zeros((clear, LANES), jnp.float32)
        return carry

    lax.fori_loop(0, table.shape[0] // clear, zero, 0)

    step = CHAINS * UNROLL

    def add(i, carry):
        for j in range(step):
            src = from_ref[i * step + j]
            dst = to_ref[i * step + j]
            into = sums[j % CHAINS]
            at = pl.ds(src, halves, stride=SUB)
            into[at, :] = into[at, :] + table[pl.ds(dst, halves, stride=SUB), :]
        return carry

    lax.fori_loop(0, edges // step, add, 0)

    def merged(base, rows, h):
        tiles = []
        for g in range(rows // SUB):
            at = pl.ds(pl.multiple_of(base + g * tall + h * SUB, SUB), SUB)
            value = sums[0][at, :]
            for s in sums[1:]:
                value = value + s[at, :]
            tiles.append(value)
        return jnp.concatenate(tiles, axis=0)

    def finish(i, carry):
        for h in range(halves):
            rows = pl.ds(pl.multiple_of(i * 32, 32), 32)
            cols = slice(h * LANES, (h + 1) * LANES)
            pre_ref[rows, cols] = self_ref[rows, cols] + merged(i * 32 * halves, 32, h)
        return carry

    lax.fori_loop(0, masters // 32, finish, 0)

    for high, back in ((0, back_x), (1, back_y)):
        for first in range(len(back)):
            for second in range(back[first].shape[0]):
                x, y, group = blocks(high, first, second)
                target = spot_ref[pl.ds(group, 1), :]
                rows = lax.broadcasted_iota(jnp.int32, (back[first].shape[1], target.shape[1]), 0)
                chosen = (rows == target).astype(jnp.float32).astype(jnp.bfloat16)
                block = jnp.concatenate(
                    [
                        jnp.concatenate(
                            [merged(base_of(x, y, high, z), slots, h) for h in range(halves)], axis=1
                        ).astype(jnp.bfloat16)
                        for z in range(deep)
                    ],
                    axis=0,
                )
                back[first][second] = jnp.dot(
                    chosen, block, preferred_element_type=jnp.float32
                ).astype(jnp.bfloat16)


def final_kernel(home_ref, pre_ref, weight_ref, grad_ref, self_ref, neigh_ref):
    hub = home_ref.shape[1]
    parts, pay, width = weight_ref.shape
    total = pre_ref[0:hub, :]
    for z in range(home_ref.shape[0]):
        total = total + home_ref[z].astype(jnp.float32)
    grad_ref[0:hub, :] = total.astype(jnp.bfloat16)
    grad_ref[hub:, :] = pre_ref[hub:, :].astype(jnp.bfloat16)
    quarter = parts // 4
    for which, ref in ((0, self_ref), (1, neigh_ref)):
        for half in range(2):

            def place(i, carry, which=which, ref=ref, half=half):
                peer = (which * 2 + half) * quarter + i
                rows = pl.ds(pl.multiple_of(i * pay, SUB), pay)
                ref[rows, half * width : (half + 1) * width] = weight_ref[peer].astype(jnp.float32)
                return carry

            lax.fori_loop(0, quarter, place, 0)


def on_device(
    features,
    grad_out,
    pre_act,
    neigh_mean,
    w_self,
    w_neigh,
    edge_from,
    edge_to,
    edge_count,
    mirror_master,
    degrees,
):
    nx, nz, ny = GRID
    deep = nz // 2
    masters, width = features.shape
    parts = lax.axis_size("dom")
    mirrors = mirror_master.shape[0]
    slots = mirrors // parts
    hub = min(masters, 64)
    local = masters + mirrors
    halves = width // LANES
    edges = edge_from.shape[0]
    contract = (((1,), (1,)), ((), ()))
    over_rows = (((0,), (0,)), ((), ()))
    first = lax.axis_index("feat") == 0

    def both(rows_out, rows_act):
        mine = (rows_out.astype(jnp.float32) * (rows_act > 0).astype(jnp.float32)).astype(jnp.bfloat16)
        other = lax.ppermute(mine, "feat", [(0, 1), (1, 0)])
        return jnp.concatenate([jnp.where(first, mine, other), jnp.where(first, other, mine)], axis=1)

    def scale(cols, degree):
        part = lax.dot_general(cols, w_neigh, contract, preferred_element_type=jnp.float32)
        return (part / degree[:, None].astype(jnp.float32)).astype(jnp.bfloat16)

    shared = scale(both(grad_out[:hub], pre_act[:hub]), degrees[:hub])
    copies = jnp.broadcast_to(shared, (nz, *shared.shape))
    column = lax.all_to_all(
        copies, "dom", split_axis=0, concat_axis=0, axis_index_groups=columns(), tiled=True
    )

    block_cols = both(grad_out, pre_act)
    grad_self = lax.dot_general(features, block_cols, over_rows, preferred_element_type=jnp.float32)
    grad_neigh = lax.dot_general(neigh_mean, block_cols, over_rows, preferred_element_type=jnp.float32)
    pay = jnp.concatenate(
        [grad_self[:, :width], grad_self[:, width:], grad_neigh[:, :width], grad_neigh[:, width:]],
        axis=0,
    ).astype(jnp.bfloat16)
    tail = pay.shape[0] // parts

    low = column[:deep].reshape(deep * hub, width)
    high = column[deep:].reshape(deep * hub, width)
    low_far = [lax.ppermute(low, "dom", ring("x", k)) for k in range(1, nx)]
    high_far = [lax.ppermute(high, "dom", ring("y", k)) for k in range(1, ny)]
    scaled = scale(block_cols, degrees)
    self_part = lax.dot_general(block_cols, w_self, contract, preferred_element_type=jnp.float32)
    low_set = jnp.stack([low] + low_far)
    high_set = jnp.stack([high] + high_far)

    low_set, high_set, pay = lax.optimization_barrier((low_set, high_set, pay))
    low_got = [low_set] + [lax.ppermute(low_set, "dom", ring("y", k)) for k in range(1, ny)]
    high_got = [high_set] + [lax.ppermute(high_set, "dom", ring("x", k)) for k in range(1, nx)]
    pieces = lax.all_to_all(
        pay.reshape(parts, tail, width), "dom", split_axis=0, concat_axis=0, tiled=True
    )

    order = mirror_master.reshape(nx, 2, deep, ny, slots).transpose(0, 3, 1, 2, 4)
    spots = order.reshape(nx * ny * 2, deep * slots) + jnp.repeat(
        jnp.arange(deep, dtype=jnp.int32) * hub, slots
    )
    chosen = pl.pallas_call(
        picks_kernel,
        out_shape=pltpu.VMEM((nx * ny * 2, deep * slots, deep * hub), jnp.bfloat16),
        in_specs=[VMEM],
        out_specs=VMEM,
        compiler_params=pltpu.CompilerParams(vmem_limit_bytes=8 << 20),
        name="picks",
    )(spots)

    def spot(row):
        return (row // SUB) * (SUB * halves) + row % SUB

    live = jnp.arange(edges, dtype=jnp.int32) < edge_count[0]
    from_at = spot(jnp.where(live, edge_from, local))
    to_at = spot(edge_to)
    me = lax.axis_index("dom")
    my_x, my_y = me // (nz * ny), me % ny
    place = jnp.concatenate(
        [(my_x - jnp.arange(nx, dtype=jnp.int32)) % nx, (my_y - jnp.arange(ny, dtype=jnp.int32)) % ny]
    ).astype(jnp.int32)

    lanes = local * halves
    low_type = pltpu.HBM(low_set.shape, jnp.bfloat16)
    high_type = pltpu.HBM(high_set.shape, jnp.bfloat16)
    results = pl.pallas_call(
        functools.partial(edge_kernel, GRID, slots),
        out_shape=[pltpu.HBM((masters, width), jnp.float32)] + [low_type] * ny + [high_type] * nx,
        in_specs=[SMEM] * 3 + [VMEM] * (4 + nx + ny),
        out_specs=[VMEM] * (1 + nx + ny),
        scratch_shapes=[pltpu.VMEM((lanes, LANES), jnp.float32)]
        + [pltpu.VMEM((lanes + SUB * halves, LANES), jnp.float32) for _ in range(CHAINS)],
        compiler_params=pltpu.CompilerParams(vmem_limit_bytes=34 << 20),
        name="edges",
    )(from_at, to_at, place, *(near(a) for a in (scaled, self_part, spots, chosen, *low_got, *high_got)))
    pre, low_back, high_back = results[0], results[1 : 1 + ny], results[1 + ny :]

    share = jnp.sum(pieces.astype(jnp.float32), axis=0).astype(jnp.bfloat16)
    low_back, high_back, share = lax.optimization_barrier((low_back, high_back, share))
    low_part = [low_back[0]] + [lax.ppermute(low_back[k], "dom", ring("y", -k)) for k in range(1, ny)]
    high_part = [high_back[0]] + [lax.ppermute(high_back[k], "dom", ring("x", -k)) for k in range(1, nx)]
    weights = lax.all_to_all(
        jnp.broadcast_to(share, (parts, *share.shape)), "dom", split_axis=0, concat_axis=0, tiled=True
    )
    low_sum = [sum_of([p[k] for p in low_part]) for k in range(nx)]
    high_sum = [sum_of([p[k] for p in high_part]) for k in range(ny)]
    low_sent = [low_sum[0]] + [
        lax.ppermute(low_sum[k].astype(jnp.bfloat16), "dom", ring("x", -k)) for k in range(1, nx)
    ]
    high_sent = [high_sum[0]] + [
        lax.ppermute(high_sum[k].astype(jnp.bfloat16), "dom", ring("y", -k)) for k in range(1, ny)
    ]
    column_sum = jnp.concatenate([sum_of(low_sent), sum_of(high_sent)], axis=0).astype(jnp.bfloat16)
    column_sum, weights, pre = lax.optimization_barrier((column_sum, weights, pre))
    home = lax.all_to_all(
        column_sum.reshape(nz, hub, width),
        "dom",
        split_axis=0,
        concat_axis=0,
        axis_index_groups=columns(),
        tiled=True,
    )
    return pl.pallas_call(
        final_kernel,
        out_shape=(
            jax.ShapeDtypeStruct((masters, width), jnp.bfloat16),
            jax.ShapeDtypeStruct(w_self.shape, jnp.float32),
            jax.ShapeDtypeStruct(w_neigh.shape, jnp.float32),
        ),
        in_specs=[VMEM] * 3,
        out_specs=[VMEM] * 3,
        compiler_params=pltpu.CompilerParams(vmem_limit_bytes=12 << 20),
        name="final",
    )(near(home), near(pre), near(weights))


def solution(mesh):
    placed = (
        P("dom", "feat"),
        P("dom", "feat"),
        P("dom", "feat"),
        P("dom", "feat"),
        P("feat", None),
        P("feat", None),
        P("dom"),
        P("dom"),
        P("dom"),
        P("dom"),
        P("dom"),
    )

    return jax.shard_map(
        on_device,
        mesh=mesh,
        in_specs=placed,
        out_specs=(P("dom", "feat"), P("feat", None), P("feat", None)),
        check_vma=False,
    )
```

```python
import functools

import jax
import jax.numpy as jnp
from jax import lax
from jax.experimental import pallas as pl
from jax.experimental.pallas import tpu as pltpu
from jax.sharding import PartitionSpec as P

LANES = 128
SUB = 8
GRID = (4, 8, 4)
CHAINS = 4
UNROLL = 8
VMEM = pl.BlockSpec(memory_space=pltpu.VMEM)
SMEM = pl.BlockSpec(memory_space=pltpu.SMEM)


def near(array):
    return pltpu.with_memory_space_constraint(array, pltpu.VMEM)


def ring(axis, shift):
    nx, nz, ny = GRID
    pairs = []
    for x in range(nx):
        for z in range(nz):
            for y in range(ny):
                tx = (x + shift) % nx if axis == "x" else x
                ty = (y + shift) % ny if axis == "y" else y
                pairs.append(((x * nz + z) * ny + y, (tx * nz + z) * ny + ty))
    return pairs


def columns():
    nx, nz, ny = GRID
    return [[(x * nz + z) * ny + y for z in range(nz)] for x in range(nx) for y in range(ny)]


def planes():
    nx, nz, ny = GRID
    return [[(x * nz + z) * ny + y for x in range(nx) for y in range(ny)] for z in range(nz)]


def swap(array, groups):
    return lax.all_to_all(array, "dom", split_axis=0, concat_axis=0, axis_index_groups=groups, tiled=True)


def sum_of(arrays):
    total = arrays[0].astype(jnp.float32)
    for a in arrays[1:]:
        total = total + a.astype(jnp.float32)
    return total


def picks_kernel(spot_ref, out_ref):
    groups, lanes = spot_ref.shape
    rows = out_ref.shape[2]

    def one(g, carry):
        spread = jnp.broadcast_to(spot_ref[pl.ds(g, 1), :].astype(jnp.float32), (LANES, lanes))
        across = jnp.concatenate([jnp.transpose(spread)] * (rows // min(rows, LANES)), axis=1)
        hub = lax.broadcasted_iota(jnp.int32, (lanes, across.shape[1]), 1).astype(jnp.float32)
        chosen = (across == hub).astype(jnp.float32).astype(jnp.bfloat16)
        out_ref[g] = chosen[:, 0:rows]
        return carry

    lax.fori_loop(0, groups, one, 0)


def edge_kernel(grid, slots, from_ref, to_ref, place_ref, own_ref, self_ref, spot_ref, pick_ref, *rest):
    nx, nz, ny = grid
    got_x = rest[0:ny]
    got_y = rest[ny : ny + nx]
    pre_ref = rest[ny + nx]
    back_x = rest[ny + nx + 1 : 2 * ny + nx + 1]
    back_y = rest[2 * ny + nx + 1 : 2 * (ny + nx) + 1]
    table = rest[2 * (ny + nx) + 1]
    sums = rest[2 * (ny + nx) + 2 :]
    masters, width = own_ref.shape
    halves = width // LANES
    tall = SUB * halves
    edges = from_ref.shape[0]
    deep = nz // 2

    def put(base, block):
        for g in range(block.shape[0] // SUB):
            for h in range(halves):
                at = pl.multiple_of(base + g * tall + h * SUB, SUB)
                table[pl.ds(at, SUB), :] = block[g * SUB : (g + 1) * SUB, h * LANES : (h + 1) * LANES]

    def own(i, carry):
        put(i * 32 * halves, own_ref[pl.ds(pl.multiple_of(i * 32, 32), 32), :].astype(jnp.float32))
        return carry

    lax.fori_loop(0, masters // 32, own, 0)

    def base_of(x, y, high, z):
        owner = (x * nz + high * deep + z) * ny + y
        return (masters + owner * slots) * halves

    def blocks(high, first, second):
        if high:
            x, y = place_ref[first], place_ref[nx + second]
        else:
            x, y = place_ref[second], place_ref[nx + first]
        return x, y, (x * ny + y) * 2 + high

    for high, got in ((0, got_x), (1, got_y)):
        for first in range(len(got)):

            def fetch(second, carry, high=high, first=first, got=got):
                x, y, group = blocks(high, first, second)
                rows = jnp.dot(pick_ref[group], got[first][second], preferred_element_type=jnp.float32)
                for z in range(deep):
                    put(base_of(x, y, high, z), rows[z * slots : (z + 1) * slots])
                return carry

            for second in range(got[first].shape[0]):
                fetch(second, 0)

    clear = 16 * SUB

    def zero(i, carry):
        for s in sums:
            s[pl.ds(pl.multiple_of(i * clear, clear), clear), :] = jnp.zeros((clear, LANES), jnp.float32)
        return carry

    lax.fori_loop(0, table.shape[0] // clear, zero, 0)

    step = CHAINS * UNROLL

    def add(i, carry):
        for j in range(step):
            src = from_ref[i * step + j]
            dst = to_ref[i * step + j]
            into = sums[j % CHAINS]
            at = pl.ds(src, halves, stride=SUB)
            into[at, :] = into[at, :] + table[pl.ds(dst, halves, stride=SUB), :]
        return carry

    lax.fori_loop(0, edges // step, add, 0)

    def merged(base, rows, h):
        tiles = []
        for g in range(rows // SUB):
            at = pl.ds(pl.multiple_of(base + g * tall + h * SUB, SUB), SUB)
            value = sums[0][at, :]
            for s in sums[1:]:
                value = value + s[at, :]
            tiles.append(value)
        return jnp.concatenate(tiles, axis=0)

    def finish(i, carry):
        for h in range(halves):
            rows = pl.ds(pl.multiple_of(i * 32, 32), 32)
            cols = slice(h * LANES, (h + 1) * LANES)
            pre_ref[rows, cols] = self_ref[rows, cols] + merged(i * 32 * halves, 32, h)
        return carry

    lax.fori_loop(0, masters // 32, finish, 0)

    for high, back in ((0, back_x), (1, back_y)):
        for first in range(len(back)):
            for second in range(back[first].shape[0]):
                x, y, group = blocks(high, first, second)
                target = spot_ref[pl.ds(group, 1), :]
                rows = lax.broadcasted_iota(jnp.int32, (back[first].shape[1], target.shape[1]), 0)
                chosen = (rows == target).astype(jnp.float32).astype(jnp.bfloat16)
                block = jnp.concatenate(
                    [
                        jnp.concatenate(
                            [merged(base_of(x, y, high, z), slots, h) for h in range(halves)], axis=1
                        ).astype(jnp.bfloat16)
                        for z in range(deep)
                    ],
                    axis=0,
                )
                back[first][second] = jnp.dot(
                    chosen, block, preferred_element_type=jnp.float32
                ).astype(jnp.bfloat16)


def final_kernel(home_ref, pre_ref, weight_ref, grad_ref, self_ref, neigh_ref):
    hub = home_ref.shape[1]
    parts, pay, width = weight_ref.shape
    total = pre_ref[0:hub, :]
    for z in range(home_ref.shape[0]):
        total = total + home_ref[z].astype(jnp.float32)
    grad_ref[0:hub, :] = total.astype(jnp.bfloat16)
    grad_ref[hub:, :] = pre_ref[hub:, :].astype(jnp.bfloat16)
    quarter = parts // 4
    for which, ref in ((0, self_ref), (1, neigh_ref)):
        for half in range(2):

            def place(i, carry, which=which, ref=ref, half=half):
                peer = (which * 2 + half) * quarter + i
                rows = pl.ds(pl.multiple_of(i * pay, SUB), pay)
                ref[rows, half * width : (half + 1) * width] = weight_ref[peer].astype(jnp.float32)
                return carry

            lax.fori_loop(0, quarter, place, 0)


def on_device(
    features,
    grad_out,
    pre_act,
    neigh_mean,
    w_self,
    w_neigh,
    edge_from,
    edge_to,
    edge_count,
    mirror_master,
    degrees,
):
    nx, nz, ny = GRID
    deep = nz // 2
    masters, width = features.shape
    parts = lax.axis_size("dom")
    mirrors = mirror_master.shape[0]
    slots = mirrors // parts
    hub = min(masters, 64)
    local = masters + mirrors
    halves = width // LANES
    edges = edge_from.shape[0]
    contract = (((1,), (1,)), ((), ()))
    over_rows = (((0,), (0,)), ((), ()))
    first = lax.axis_index("feat") == 0

    def both(rows_out, rows_act):
        mine = (rows_out.astype(jnp.float32) * (rows_act > 0).astype(jnp.float32)).astype(jnp.bfloat16)
        other = lax.ppermute(mine, "feat", [(0, 1), (1, 0)])
        return jnp.concatenate([jnp.where(first, mine, other), jnp.where(first, other, mine)], axis=1)

    def scale(cols, degree):
        part = lax.dot_general(cols, w_neigh, contract, preferred_element_type=jnp.float32)
        return (part / degree[:, None].astype(jnp.float32)).astype(jnp.bfloat16)

    shared = scale(both(grad_out[:hub], pre_act[:hub]), degrees[:hub])
    copies = jnp.broadcast_to(shared, (nz, *shared.shape))
    column = lax.all_to_all(
        copies, "dom", split_axis=0, concat_axis=0, axis_index_groups=columns(), tiled=True
    )

    block_cols = both(grad_out, pre_act)
    grad_self = lax.dot_general(features, block_cols, over_rows, preferred_element_type=jnp.float32)
    grad_neigh = lax.dot_general(neigh_mean, block_cols, over_rows, preferred_element_type=jnp.float32)
    pay = jnp.concatenate(
        [grad_self[:, :width], grad_self[:, width:], grad_neigh[:, :width], grad_neigh[:, width:]],
        axis=0,
    ).astype(jnp.bfloat16)
    tail = pay.shape[0] // parts

    low = column[:deep].reshape(deep * hub, width)
    high = column[deep:].reshape(deep * hub, width)
    low_far = [lax.ppermute(low, "dom", ring("x", k)) for k in range(1, nx)]
    high_far = [lax.ppermute(high, "dom", ring("y", k)) for k in range(1, ny)]
    scaled = scale(block_cols, degrees)
    self_part = lax.dot_general(block_cols, w_self, contract, preferred_element_type=jnp.float32)
    low_set = jnp.stack([low] + low_far)
    high_set = jnp.stack([high] + high_far)

    low_set, high_set, pay = lax.optimization_barrier((low_set, high_set, pay))
    low_got = [low_set] + [lax.ppermute(low_set, "dom", ring("y", k)) for k in range(1, ny)]
    high_got = [high_set] + [lax.ppermute(high_set, "dom", ring("x", k)) for k in range(1, nx)]
    pieces = swap(pay.reshape(nz, -1, width), columns())
    pieces = swap(jnp.sum(pieces.astype(jnp.float32), axis=0).reshape(nx * ny, tail, width), planes())

    order = mirror_master.reshape(nx, 2, deep, ny, slots).transpose(0, 3, 1, 2, 4)
    spots = order.reshape(nx * ny * 2, deep * slots) + jnp.repeat(
        jnp.arange(deep, dtype=jnp.int32) * hub, slots
    )
    chosen = pl.pallas_call(
        picks_kernel,
        out_shape=pltpu.VMEM((nx * ny * 2, deep * slots, deep * hub), jnp.bfloat16),
        in_specs=[VMEM],
        out_specs=VMEM,
        compiler_params=pltpu.CompilerParams(vmem_limit_bytes=8 << 20),
        name="picks",
    )(spots)

    def spot(row):
        return (row // SUB) * (SUB * halves) + row % SUB

    live = jnp.arange(edges, dtype=jnp.int32) < edge_count[0]
    from_at = spot(jnp.where(live, edge_from, local))
    to_at = spot(edge_to)
    me = lax.axis_index("dom")
    my_x, my_y = me // (nz * ny), me % ny
    place = jnp.concatenate(
        [(my_x - jnp.arange(nx, dtype=jnp.int32)) % nx, (my_y - jnp.arange(ny, dtype=jnp.int32)) % ny]
    ).astype(jnp.int32)

    lanes = local * halves
    low_type = pltpu.HBM(low_set.shape, jnp.bfloat16)
    high_type = pltpu.HBM(high_set.shape, jnp.bfloat16)
    edge_call = pl.pallas_call(
        functools.partial(edge_kernel, GRID, slots),
        out_shape=[pltpu.HBM((masters, width), jnp.float32)] + [low_type] * ny + [high_type] * nx,
        in_specs=[SMEM] * 3 + [VMEM] * (4 + nx + ny),
        out_specs=[VMEM] * (1 + nx + ny),
        scratch_shapes=[pltpu.VMEM((lanes, LANES), jnp.float32)]
        + [pltpu.VMEM((lanes + SUB * halves, LANES), jnp.float32) for _ in range(CHAINS)],
        compiler_params=pltpu.CompilerParams(vmem_limit_bytes=34 << 20),
        name="edges",
    )
    results = edge_call(from_at, to_at, place, *(near(a) for a in (scaled, self_part, spots, chosen, *low_got, *high_got)))
    pre, low_back, high_back = results[0], results[1 : 1 + ny], results[1 + ny :]

    share = jnp.sum(pieces, axis=0).astype(jnp.bfloat16)
    low_back, high_back, share = lax.optimization_barrier((low_back, high_back, share))
    low_part = [low_back[0]] + [lax.ppermute(low_back[k], "dom", ring("y", -k)) for k in range(1, ny)]
    high_part = [high_back[0]] + [lax.ppermute(high_back[k], "dom", ring("x", -k)) for k in range(1, nx)]
    weights = swap(jnp.broadcast_to(share, (nx * ny, *share.shape)), planes()).reshape(-1, width)
    weights = swap(jnp.broadcast_to(weights, (nz, *weights.shape)), columns()).reshape(parts, tail, width)
    low_sum = [sum_of([p[k] for p in low_part]) for k in range(nx)]
    high_sum = [sum_of([p[k] for p in high_part]) for k in range(ny)]
    low_sent = [low_sum[0]] + [
        lax.ppermute(low_sum[k].astype(jnp.bfloat16), "dom", ring("x", -k)) for k in range(1, nx)
    ]
    high_sent = [high_sum[0]] + [
        lax.ppermute(high_sum[k].astype(jnp.bfloat16), "dom", ring("y", -k)) for k in range(1, ny)
    ]
    column_sum = jnp.concatenate([sum_of(low_sent), sum_of(high_sent)], axis=0).astype(jnp.bfloat16)
    column_sum, weights, pre = lax.optimization_barrier((column_sum, weights, pre))
    home = lax.all_to_all(
        column_sum.reshape(nz, hub, width),
        "dom",
        split_axis=0,
        concat_axis=0,
        axis_index_groups=columns(),
        tiled=True,
    )
    return pl.pallas_call(
        final_kernel,
        out_shape=(
            jax.ShapeDtypeStruct((masters, width), jnp.bfloat16),
            jax.ShapeDtypeStruct(w_self.shape, jnp.float32),
            jax.ShapeDtypeStruct(w_neigh.shape, jnp.float32),
        ),
        in_specs=[VMEM] * 3,
        out_specs=[VMEM] * 3,
        compiler_params=pltpu.CompilerParams(vmem_limit_bytes=12 << 20),
        name="final",
    )(near(home), near(pre), near(weights))


def solution(mesh):
    placed = (
        P("dom", "feat"),
        P("dom", "feat"),
        P("dom", "feat"),
        P("dom", "feat"),
        P("feat", None),
        P("feat", None),
        P("dom"),
        P("dom"),
        P("dom"),
        P("dom"),
        P("dom"),
    )

    return jax.shard_map(
        on_device,
        mesh=mesh,
        in_specs=placed,
        out_specs=(P("dom", "feat"), P("feat", None), P("feat", None)),
        check_vma=False,
    )
```

```python
import functools

import jax
import jax.numpy as jnp
from jax import lax
from jax.experimental import pallas as pl
from jax.experimental.pallas import tpu as pltpu
from jax.sharding import PartitionSpec as P

LANES = 128
SUB = 8
GRID = (4, 8, 4)
CHAINS = 4
UNROLL = 8
VMEM = pl.BlockSpec(memory_space=pltpu.VMEM)
SMEM = pl.BlockSpec(memory_space=pltpu.SMEM)


def near(array):
    return pltpu.with_memory_space_constraint(array, pltpu.VMEM)


def ring(axis, shift):
    nx, nz, ny = GRID
    pairs = []
    for x in range(nx):
        for z in range(nz):
            for y in range(ny):
                tx = (x + shift) % nx if axis == "x" else x
                ty = (y + shift) % ny if axis == "y" else y
                pairs.append(((x * nz + z) * ny + y, (tx * nz + z) * ny + ty))
    return pairs


def columns():
    nx, nz, ny = GRID
    return [[(x * nz + z) * ny + y for z in range(nz)] for x in range(nx) for y in range(ny)]


def planes():
    nx, nz, ny = GRID
    return [[(x * nz + z) * ny + y for x in range(nx) for y in range(ny)] for z in range(nz)]


def swap(array, groups):
    return lax.all_to_all(array, "dom", split_axis=0, concat_axis=0, axis_index_groups=groups, tiled=True)


def sum_of(arrays):
    total = arrays[0].astype(jnp.float32)
    for a in arrays[1:]:
        total = total + a.astype(jnp.float32)
    return total


def picks_kernel(spot_ref, out_ref):
    groups, lanes = spot_ref.shape
    rows = out_ref.shape[2]

    def one(g, carry):
        spread = jnp.broadcast_to(spot_ref[pl.ds(g, 1), :].astype(jnp.float32), (LANES, lanes))
        across = jnp.concatenate([jnp.transpose(spread)] * (rows // min(rows, LANES)), axis=1)
        hub = lax.broadcasted_iota(jnp.int32, (lanes, across.shape[1]), 1).astype(jnp.float32)
        chosen = (across == hub).astype(jnp.float32).astype(jnp.bfloat16)
        out_ref[g] = chosen[:, 0:rows]
        return carry

    lax.fori_loop(0, groups, one, 0)


def edge_kernel(grid, slots, from_ref, to_ref, place_ref, own_ref, self_ref, spot_ref, pick_ref, *rest):
    nx, nz, ny = grid
    got_x = rest[0:ny]
    got_y = rest[ny : ny + nx]
    pre_ref = rest[ny + nx]
    back_x = rest[ny + nx + 1 : 2 * ny + nx + 1]
    back_y = rest[2 * ny + nx + 1 : 2 * (ny + nx) + 1]
    table = rest[2 * (ny + nx) + 1]
    sums = rest[2 * (ny + nx) + 2 :]
    masters, width = own_ref.shape
    halves = width // LANES
    tall = SUB * halves
    edges = from_ref.shape[0]
    deep = nz // 2

    def put(base, block):
        for g in range(block.shape[0] // SUB):
            for h in range(halves):
                at = pl.multiple_of(base + g * tall + h * SUB, SUB)
                table[pl.ds(at, SUB), :] = block[g * SUB : (g + 1) * SUB, h * LANES : (h + 1) * LANES]

    def own(i, carry):
        put(i * 32 * halves, own_ref[pl.ds(pl.multiple_of(i * 32, 32), 32), :].astype(jnp.float32))
        return carry

    lax.fori_loop(0, masters // 32, own, 0)

    def base_of(x, y, high, z):
        owner = (x * nz + high * deep + z) * ny + y
        return (masters + owner * slots) * halves

    def blocks(high, first, second):
        if high:
            x, y = place_ref[first], place_ref[nx + second]
        else:
            x, y = place_ref[second], place_ref[nx + first]
        return x, y, (x * ny + y) * 2 + high

    for high, got in ((0, got_x), (1, got_y)):
        for first in range(len(got)):

            def fetch(second, carry, high=high, first=first, got=got):
                x, y, group = blocks(high, first, second)
                rows = jnp.dot(pick_ref[group], got[first][second], preferred_element_type=jnp.float32)
                for z in range(deep):
                    put(base_of(x, y, high, z), rows[z * slots : (z + 1) * slots])
                return carry

            for second in range(got[first].shape[0]):
                fetch(second, 0)

    clear = 16 * SUB

    def zero(i, carry):
        for s in sums:
            s[pl.ds(pl.multiple_of(i * clear, clear), clear), :] = jnp.zeros((clear, LANES), jnp.float32)
        return carry

    lax.fori_loop(0, table.shape[0] // clear, zero, 0)

    step = CHAINS * UNROLL

    def add(i, carry):
        for j in range(step):
            src = from_ref[i * step + j]
            dst = to_ref[i * step + j]
            into = sums[j % CHAINS]
            at = pl.ds(src, halves, stride=SUB)
            into[at, :] = into[at, :] + table[pl.ds(dst, halves, stride=SUB), :]
        return carry

    lax.fori_loop(0, edges // step, add, 0)

    def merged(base, rows, h):
        tiles = []
        for g in range(rows // SUB):
            at = pl.ds(pl.multiple_of(base + g * tall + h * SUB, SUB), SUB)
            value = sums[0][at, :]
            for s in sums[1:]:
                value = value + s[at, :]
            tiles.append(value)
        return jnp.concatenate(tiles, axis=0)

    def finish(i, carry):
        for h in range(halves):
            rows = pl.ds(pl.multiple_of(i * 32, 32), 32)
            cols = slice(h * LANES, (h + 1) * LANES)
            pre_ref[rows, cols] = self_ref[rows, cols] + merged(i * 32 * halves, 32, h)
        return carry

    lax.fori_loop(0, masters // 32, finish, 0)

    for high, back in ((0, back_x), (1, back_y)):
        for first in range(len(back)):
            for second in range(back[first].shape[0]):
                x, y, group = blocks(high, first, second)
                target = spot_ref[pl.ds(group, 1), :]
                rows = lax.broadcasted_iota(jnp.int32, (back[first].shape[1], target.shape[1]), 0)
                chosen = (rows == target).astype(jnp.float32).astype(jnp.bfloat16)
                block = jnp.concatenate(
                    [
                        jnp.concatenate(
                            [merged(base_of(x, y, high, z), slots, h) for h in range(halves)], axis=1
                        ).astype(jnp.bfloat16)
                        for z in range(deep)
                    ],
                    axis=0,
                )
                back[first][second] = jnp.dot(
                    chosen, block, preferred_element_type=jnp.float32
                ).astype(jnp.bfloat16)


def final_kernel(home_ref, pre_ref, weight_ref, grad_ref, self_ref, neigh_ref):
    hub = home_ref.shape[1]
    parts, pay, width = weight_ref.shape
    total = pre_ref[0:hub, :]
    for z in range(home_ref.shape[0]):
        total = total + home_ref[z].astype(jnp.float32)
    grad_ref[0:hub, :] = total.astype(jnp.bfloat16)
    grad_ref[hub:, :] = pre_ref[hub:, :].astype(jnp.bfloat16)
    quarter = parts // 4
    for which, ref in ((0, self_ref), (1, neigh_ref)):
        for half in range(2):

            def place(i, carry, which=which, ref=ref, half=half):
                peer = (which * 2 + half) * quarter + i
                rows = pl.ds(pl.multiple_of(i * pay, SUB), pay)
                ref[rows, half * width : (half + 1) * width] = weight_ref[peer].astype(jnp.float32)
                return carry

            lax.fori_loop(0, quarter, place, 0)


def on_device(
    features,
    grad_out,
    pre_act,
    neigh_mean,
    w_self,
    w_neigh,
    edge_from,
    edge_to,
    edge_count,
    mirror_master,
    degrees,
):
    nx, nz, ny = GRID
    deep = nz // 2
    masters, width = features.shape
    parts = lax.axis_size("dom")
    mirrors = mirror_master.shape[0]
    slots = mirrors // parts
    hub = min(masters, 64)
    local = masters + mirrors
    halves = width // LANES
    edges = edge_from.shape[0]
    contract = (((1,), (1,)), ((), ()))
    over_rows = (((0,), (0,)), ((), ()))
    first = lax.axis_index("feat") == 0

    def both(rows_out, rows_act):
        mine = (rows_out.astype(jnp.float32) * (rows_act > 0).astype(jnp.float32)).astype(jnp.bfloat16)
        other = lax.ppermute(mine, "feat", [(0, 1), (1, 0)])
        return jnp.concatenate([jnp.where(first, mine, other), jnp.where(first, other, mine)], axis=1)

    def scale(cols, degree):
        part = lax.dot_general(cols, w_neigh, contract, preferred_element_type=jnp.float32)
        return (part / degree[:, None].astype(jnp.float32)).astype(jnp.bfloat16)

    shared = scale(both(grad_out[:hub], pre_act[:hub]), degrees[:hub])
    copies = jnp.broadcast_to(shared, (nz, *shared.shape))
    column = lax.all_to_all(
        copies, "dom", split_axis=0, concat_axis=0, axis_index_groups=columns(), tiled=True
    )

    block_cols = both(grad_out, pre_act)
    grad_self = lax.dot_general(features, block_cols, over_rows, preferred_element_type=jnp.float32)
    grad_neigh = lax.dot_general(neigh_mean, block_cols, over_rows, preferred_element_type=jnp.float32)
    pay = jnp.concatenate(
        [grad_self[:, :width], grad_self[:, width:], grad_neigh[:, :width], grad_neigh[:, width:]],
        axis=0,
    ).astype(jnp.bfloat16)
    tail = pay.shape[0] // parts

    low = column[:deep].reshape(deep * hub, width)
    high = column[deep:].reshape(deep * hub, width)
    low_far = [lax.ppermute(low, "dom", ring("x", k)) for k in range(1, nx)]
    high_far = [lax.ppermute(high, "dom", ring("y", k)) for k in range(1, ny)]
    pieces = swap(pay.reshape(nz, -1, width), columns())
    low_set = jnp.stack([low] + low_far)
    high_set = jnp.stack([high] + high_far)
    low_got = [low_set] + [lax.ppermute(low_set, "dom", ring("y", k)) for k in range(1, ny)]
    high_got = [high_set] + [lax.ppermute(high_set, "dom", ring("x", k)) for k in range(1, nx)]
    scaled = scale(block_cols, degrees)
    self_part = lax.dot_general(block_cols, w_self, contract, preferred_element_type=jnp.float32)
    chunk = jnp.sum(pieces.astype(jnp.float32), axis=0).astype(jnp.bfloat16)
    chunks = jnp.broadcast_to(chunk, (nx * ny, *chunk.shape))
    chunks = swap(chunks, planes())

    order = mirror_master.reshape(nx, 2, deep, ny, slots).transpose(0, 3, 1, 2, 4)
    spots = order.reshape(nx * ny * 2, deep * slots) + jnp.repeat(
        jnp.arange(deep, dtype=jnp.int32) * hub, slots
    )
    chosen = pl.pallas_call(
        picks_kernel,
        out_shape=pltpu.VMEM((nx * ny * 2, deep * slots, deep * hub), jnp.bfloat16),
        in_specs=[VMEM],
        out_specs=VMEM,
        compiler_params=pltpu.CompilerParams(vmem_limit_bytes=8 << 20),
        name="picks",
    )(spots)

    def spot(row):
        return (row // SUB) * (SUB * halves) + row % SUB

    live = jnp.arange(edges, dtype=jnp.int32) < edge_count[0]
    from_at = spot(jnp.where(live, edge_from, local))
    to_at = spot(edge_to)
    me = lax.axis_index("dom")
    my_x, my_y = me // (nz * ny), me % ny
    place = jnp.concatenate(
        [(my_x - jnp.arange(nx, dtype=jnp.int32)) % nx, (my_y - jnp.arange(ny, dtype=jnp.int32)) % ny]
    ).astype(jnp.int32)

    lanes = local * halves
    low_type = pltpu.HBM(low_set.shape, jnp.bfloat16)
    high_type = pltpu.HBM(high_set.shape, jnp.bfloat16)
    edge_call = pl.pallas_call(
        functools.partial(edge_kernel, GRID, slots),
        out_shape=[pltpu.HBM((masters, width), jnp.float32)] + [low_type] * ny + [high_type] * nx,
        in_specs=[SMEM] * 3 + [VMEM] * (4 + nx + ny),
        out_specs=[VMEM] * (1 + nx + ny),
        scratch_shapes=[pltpu.VMEM((lanes, LANES), jnp.float32)]
        + [pltpu.VMEM((lanes + SUB * halves, LANES), jnp.float32) for _ in range(CHAINS)],
        compiler_params=pltpu.CompilerParams(vmem_limit_bytes=34 << 20),
        name="edges",
    )
    results = edge_call(from_at, to_at, place, *(near(a) for a in (scaled, self_part, spots, chosen, *low_got, *high_got)))
    pre, low_back, high_back = results[0], results[1 : 1 + ny], results[1 + ny :]

    share = jnp.sum(chunks.astype(jnp.float32), axis=0).astype(jnp.bfloat16)
    low_back, high_back, share = lax.optimization_barrier((low_back, high_back, share))
    low_part = [low_back[0]] + [lax.ppermute(low_back[k], "dom", ring("y", -k)) for k in range(1, ny)]
    high_part = [high_back[0]] + [lax.ppermute(high_back[k], "dom", ring("x", -k)) for k in range(1, nx)]
    weights = swap(jnp.broadcast_to(share, (nz, *share.shape)), columns()).reshape(parts, tail, width)
    low_sum = [sum_of([p[k] for p in low_part]) for k in range(nx)]
    high_sum = [sum_of([p[k] for p in high_part]) for k in range(ny)]
    low_sent = [low_sum[0]] + [
        lax.ppermute(low_sum[k].astype(jnp.bfloat16), "dom", ring("x", -k)) for k in range(1, nx)
    ]
    high_sent = [high_sum[0]] + [
        lax.ppermute(high_sum[k].astype(jnp.bfloat16), "dom", ring("y", -k)) for k in range(1, ny)
    ]
    column_sum = jnp.concatenate([sum_of(low_sent), sum_of(high_sent)], axis=0).astype(jnp.bfloat16)
    column_sum, weights, pre = lax.optimization_barrier((column_sum, weights, pre))
    home = lax.all_to_all(
        column_sum.reshape(nz, hub, width),
        "dom",
        split_axis=0,
        concat_axis=0,
        axis_index_groups=columns(),
        tiled=True,
    )
    return pl.pallas_call(
        final_kernel,
        out_shape=(
            jax.ShapeDtypeStruct((masters, width), jnp.bfloat16),
            jax.ShapeDtypeStruct(w_self.shape, jnp.float32),
            jax.ShapeDtypeStruct(w_neigh.shape, jnp.float32),
        ),
        in_specs=[VMEM] * 3,
        out_specs=[VMEM] * 3,
        compiler_params=pltpu.CompilerParams(vmem_limit_bytes=12 << 20),
        name="final",
    )(near(home), near(pre), near(weights))


def solution(mesh):
    placed = (
        P("dom", "feat"),
        P("dom", "feat"),
        P("dom", "feat"),
        P("dom", "feat"),
        P("feat", None),
        P("feat", None),
        P("dom"),
        P("dom"),
        P("dom"),
        P("dom"),
        P("dom"),
    )

    return jax.shard_map(
        on_device,
        mesh=mesh,
        in_specs=placed,
        out_specs=(P("dom", "feat"), P("feat", None), P("feat", None)),
        check_vma=False,
    )
```

```python
import functools

import jax
import jax.numpy as jnp
from jax import lax
from jax.experimental import pallas as pl
from jax.experimental.pallas import tpu as pltpu
from jax.sharding import PartitionSpec as P

LANES = 128
SUB = 8
GRID = (4, 8, 4)
CHAINS = 4
UNROLL = 8
VMEM = pl.BlockSpec(memory_space=pltpu.VMEM)
SMEM = pl.BlockSpec(memory_space=pltpu.SMEM)


def near(array):
    return pltpu.with_memory_space_constraint(array, pltpu.VMEM)


def far(array):
    return pltpu.with_memory_space_constraint(array, pltpu.HBM)


def ring(axis, shift):
    nx, nz, ny = GRID
    pairs = []
    for x in range(nx):
        for z in range(nz):
            for y in range(ny):
                tx = (x + shift) % nx if axis == "x" else x
                ty = (y + shift) % ny if axis == "y" else y
                pairs.append(((x * nz + z) * ny + y, (tx * nz + z) * ny + ty))
    return pairs


def columns():
    nx, nz, ny = GRID
    return [[(x * nz + z) * ny + y for z in range(nz)] for x in range(nx) for y in range(ny)]


def planes():
    nx, nz, ny = GRID
    return [[(x * nz + z) * ny + y for x in range(nx) for y in range(ny)] for z in range(nz)]


def swap(array, groups):
    return lax.all_to_all(array, "dom", split_axis=0, concat_axis=0, axis_index_groups=groups, tiled=True)


def sum_of(arrays):
    total = arrays[0].astype(jnp.float32)
    for a in arrays[1:]:
        total = total + a.astype(jnp.float32)
    return total


def picks_kernel(spot_ref, out_ref):
    groups, lanes = spot_ref.shape
    rows = out_ref.shape[2]

    def one(g, carry):
        spread = jnp.broadcast_to(spot_ref[pl.ds(g, 1), :].astype(jnp.float32), (LANES, lanes))
        across = jnp.concatenate([jnp.transpose(spread)] * (rows // min(rows, LANES)), axis=1)
        hub = lax.broadcasted_iota(jnp.int32, (lanes, across.shape[1]), 1).astype(jnp.float32)
        chosen = (across == hub).astype(jnp.float32).astype(jnp.bfloat16)
        out_ref[g] = chosen[:, 0:rows]
        return carry

    lax.fori_loop(0, groups, one, 0)


def edge_kernel(grid, slots, from_ref, to_ref, place_ref, own_ref, self_ref, spot_ref, pick_ref, *rest):
    nx, nz, ny = grid
    got_x = rest[0:ny]
    got_y = rest[ny : ny + nx]
    pre_ref = rest[ny + nx]
    back_x = rest[ny + nx + 1 : 2 * ny + nx + 1]
    back_y = rest[2 * ny + nx + 1 : 2 * (ny + nx) + 1]
    table = rest[2 * (ny + nx) + 1]
    sums = rest[2 * (ny + nx) + 2 :]
    masters, width = own_ref.shape
    halves = width // LANES
    tall = SUB * halves
    edges = from_ref.shape[0]
    deep = nz // 2

    def put(base, block):
        for g in range(block.shape[0] // SUB):
            for h in range(halves):
                at = pl.multiple_of(base + g * tall + h * SUB, SUB)
                table[pl.ds(at, SUB), :] = block[g * SUB : (g + 1) * SUB, h * LANES : (h + 1) * LANES]

    def own(i, carry):
        put(i * 32 * halves, own_ref[pl.ds(pl.multiple_of(i * 32, 32), 32), :].astype(jnp.float32))
        return carry

    lax.fori_loop(0, masters // 32, own, 0)

    def base_of(x, y, high, z):
        owner = (x * nz + high * deep + z) * ny + y
        return (masters + owner * slots) * halves

    def blocks(high, first, second):
        if high:
            x, y = place_ref[first], place_ref[nx + second]
        else:
            x, y = place_ref[second], place_ref[nx + first]
        return x, y, (x * ny + y) * 2 + high

    for high, got in ((0, got_x), (1, got_y)):
        for first in range(len(got)):

            def fetch(second, carry, high=high, first=first, got=got):
                x, y, group = blocks(high, first, second)
                rows = jnp.dot(pick_ref[group], got[first][second], preferred_element_type=jnp.float32)
                for z in range(deep):
                    put(base_of(x, y, high, z), rows[z * slots : (z + 1) * slots])
                return carry

            for second in range(got[first].shape[0]):
                fetch(second, 0)

    clear = 16 * SUB

    def zero(i, carry):
        for s in sums:
            s[pl.ds(pl.multiple_of(i * clear, clear), clear), :] = jnp.zeros((clear, LANES), jnp.float32)
        return carry

    lax.fori_loop(0, table.shape[0] // clear, zero, 0)

    step = CHAINS * UNROLL

    def add(i, carry):
        for j in range(step):
            src = from_ref[i * step + j]
            dst = to_ref[i * step + j]
            into = sums[j % CHAINS]
            at = pl.ds(src, halves, stride=SUB)
            into[at, :] = into[at, :] + table[pl.ds(dst, halves, stride=SUB), :]
        return carry

    lax.fori_loop(0, edges // step, add, 0)

    def merged(base, rows, h):
        tiles = []
        for g in range(rows // SUB):
            at = pl.ds(pl.multiple_of(base + g * tall + h * SUB, SUB), SUB)
            value = sums[0][at, :]
            for s in sums[1:]:
                value = value + s[at, :]
            tiles.append(value)
        return jnp.concatenate(tiles, axis=0)

    def finish(i, carry):
        for h in range(halves):
            rows = pl.ds(pl.multiple_of(i * 32, 32), 32)
            cols = slice(h * LANES, (h + 1) * LANES)
            pre_ref[rows, cols] = self_ref[rows, cols] + merged(i * 32 * halves, 32, h)
        return carry

    lax.fori_loop(0, masters // 32, finish, 0)

    for high, back in ((0, back_x), (1, back_y)):
        for first in range(len(back)):
            for second in range(back[first].shape[0]):
                x, y, group = blocks(high, first, second)
                target = spot_ref[pl.ds(group, 1), :]
                rows = lax.broadcasted_iota(jnp.int32, (back[first].shape[1], target.shape[1]), 0)
                chosen = (rows == target).astype(jnp.float32).astype(jnp.bfloat16)
                block = jnp.concatenate(
                    [
                        jnp.concatenate(
                            [merged(base_of(x, y, high, z), slots, h) for h in range(halves)], axis=1
                        ).astype(jnp.bfloat16)
                        for z in range(deep)
                    ],
                    axis=0,
                )
                back[first][second] = jnp.dot(
                    chosen, block, preferred_element_type=jnp.float32
                ).astype(jnp.bfloat16)


def final_kernel(home_ref, pre_ref, weight_ref, grad_ref, self_ref, neigh_ref):
    hub = home_ref.shape[1]
    parts, pay, width = weight_ref.shape
    total = pre_ref[0:hub, :]
    for z in range(home_ref.shape[0]):
        total = total + home_ref[z].astype(jnp.float32)
    grad_ref[0:hub, :] = total.astype(jnp.bfloat16)
    grad_ref[hub:, :] = pre_ref[hub:, :].astype(jnp.bfloat16)
    quarter = parts // 4
    for which, ref in ((0, self_ref), (1, neigh_ref)):
        for half in range(2):

            def place(i, carry, which=which, ref=ref, half=half):
                peer = (which * 2 + half) * quarter + i
                rows = pl.ds(pl.multiple_of(i * pay, SUB), pay)
                ref[rows, half * width : (half + 1) * width] = weight_ref[peer].astype(jnp.float32)
                return carry

            lax.fori_loop(0, quarter, place, 0)


def on_device(
    features,
    grad_out,
    pre_act,
    neigh_mean,
    w_self,
    w_neigh,
    edge_from,
    edge_to,
    edge_count,
    mirror_master,
    degrees,
):
    nx, nz, ny = GRID
    deep = nz // 2
    masters, width = features.shape
    parts = lax.axis_size("dom")
    mirrors = mirror_master.shape[0]
    slots = mirrors // parts
    hub = min(masters, 64)
    local = masters + mirrors
    halves = width // LANES
    edges = edge_from.shape[0]
    contract = (((1,), (1,)), ((), ()))
    over_rows = (((0,), (0,)), ((), ()))
    first = lax.axis_index("feat") == 0

    def both(rows_out, rows_act):
        mine = (rows_out.astype(jnp.float32) * (rows_act > 0).astype(jnp.float32)).astype(jnp.bfloat16)
        other = lax.ppermute(mine, "feat", [(0, 1), (1, 0)])
        return jnp.concatenate([jnp.where(first, mine, other), jnp.where(first, other, mine)], axis=1)

    def scale(cols, degree):
        part = lax.dot_general(cols, w_neigh, contract, preferred_element_type=jnp.float32)
        return (part / degree[:, None].astype(jnp.float32)).astype(jnp.bfloat16)

    shared = scale(both(grad_out[:hub], pre_act[:hub]), degrees[:hub])
    copies = jnp.broadcast_to(shared, (nz, *shared.shape))
    column = lax.all_to_all(
        copies, "dom", split_axis=0, concat_axis=0, axis_index_groups=columns(), tiled=True
    )

    block_cols = both(grad_out, pre_act)
    grad_self = lax.dot_general(features, block_cols, over_rows, preferred_element_type=jnp.float32)
    grad_neigh = lax.dot_general(neigh_mean, block_cols, over_rows, preferred_element_type=jnp.float32)
    pay = jnp.concatenate(
        [grad_self[:, :width], grad_self[:, width:], grad_neigh[:, :width], grad_neigh[:, width:]],
        axis=0,
    ).astype(jnp.bfloat16)
    tail = pay.shape[0] // parts

    low = column[:deep].reshape(deep * hub, width)
    high = column[deep:].reshape(deep * hub, width)
    low_far = [lax.ppermute(low, "dom", ring("x", k)) for k in range(1, nx)]
    high_far = [lax.ppermute(high, "dom", ring("y", k)) for k in range(1, ny)]
    pieces = swap(pay.reshape(nz, -1, width), columns())
    low_set = jnp.stack([low] + low_far)
    high_set = jnp.stack([high] + high_far)
    low_got = [low_set] + [lax.ppermute(low_set, "dom", ring("y", k)) for k in range(1, ny)]
    high_got = [high_set] + [lax.ppermute(high_set, "dom", ring("x", k)) for k in range(1, nx)]
    scaled = scale(block_cols, degrees)
    self_part = lax.dot_general(block_cols, w_self, contract, preferred_element_type=jnp.float32)
    chunk = jnp.sum(pieces.astype(jnp.float32), axis=0).astype(jnp.bfloat16)
    chunks = jnp.broadcast_to(chunk, (nx * ny, *chunk.shape))
    chunks = swap(chunks, planes())

    order = mirror_master.reshape(nx, 2, deep, ny, slots).transpose(0, 3, 1, 2, 4)
    spots = order.reshape(nx * ny * 2, deep * slots) + jnp.repeat(
        jnp.arange(deep, dtype=jnp.int32) * hub, slots
    )
    chosen = pl.pallas_call(
        picks_kernel,
        out_shape=pltpu.VMEM((nx * ny * 2, deep * slots, deep * hub), jnp.bfloat16),
        in_specs=[VMEM],
        out_specs=VMEM,
        compiler_params=pltpu.CompilerParams(vmem_limit_bytes=8 << 20),
        name="picks",
    )(spots)

    def spot(row):
        return (row // SUB) * (SUB * halves) + row % SUB

    live = jnp.arange(edges, dtype=jnp.int32) < edge_count[0]
    from_at = spot(jnp.where(live, edge_from, local))
    to_at = spot(edge_to)
    me = lax.axis_index("dom")
    my_x, my_y = me // (nz * ny), me % ny
    place = jnp.concatenate(
        [(my_x - jnp.arange(nx, dtype=jnp.int32)) % nx, (my_y - jnp.arange(ny, dtype=jnp.int32)) % ny]
    ).astype(jnp.int32)

    lanes = local * halves
    low_type = pltpu.HBM(low_set.shape, jnp.bfloat16)
    high_type = pltpu.HBM(high_set.shape, jnp.bfloat16)
    edge_call = pl.pallas_call(
        functools.partial(edge_kernel, GRID, slots),
        out_shape=[pltpu.HBM((masters, width), jnp.float32)] + [low_type] * ny + [high_type] * nx,
        in_specs=[SMEM] * 3 + [VMEM] * (4 + nx + ny),
        out_specs=[VMEM] * (1 + nx + ny),
        scratch_shapes=[pltpu.VMEM((lanes, LANES), jnp.float32)]
        + [pltpu.VMEM((lanes + SUB * halves, LANES), jnp.float32) for _ in range(CHAINS)],
        compiler_params=pltpu.CompilerParams(vmem_limit_bytes=42 << 20),
        name="edges",
    )
    results = edge_call(from_at, to_at, place, far(scaled), far(self_part), near(spots), near(chosen), *low_got, *high_got)
    pre, low_back, high_back = results[0], results[1 : 1 + ny], results[1 + ny :]

    share = jnp.sum(chunks.astype(jnp.float32), axis=0).astype(jnp.bfloat16)
    low_part = [low_back[0]] + [lax.ppermute(low_back[k], "dom", ring("y", -k)) for k in range(1, ny)]
    high_part = [high_back[0]] + [lax.ppermute(high_back[k], "dom", ring("x", -k)) for k in range(1, nx)]
    weights = swap(jnp.broadcast_to(share, (nz, *share.shape)), columns()).reshape(parts, tail, width)
    low_sum = [sum_of([p[k] for p in low_part]) for k in range(nx)]
    high_sum = [sum_of([p[k] for p in high_part]) for k in range(ny)]
    low_sent = [low_sum[0]] + [
        lax.ppermute(low_sum[k].astype(jnp.bfloat16), "dom", ring("x", -k)) for k in range(1, nx)
    ]
    high_sent = [high_sum[0]] + [
        lax.ppermute(high_sum[k].astype(jnp.bfloat16), "dom", ring("y", -k)) for k in range(1, ny)
    ]
    column_sum = jnp.concatenate([sum_of(low_sent), sum_of(high_sent)], axis=0).astype(jnp.bfloat16)
    column_sum, weights, pre = lax.optimization_barrier((column_sum, weights, pre))
    home = lax.all_to_all(
        column_sum.reshape(nz, hub, width),
        "dom",
        split_axis=0,
        concat_axis=0,
        axis_index_groups=columns(),
        tiled=True,
    )
    return pl.pallas_call(
        final_kernel,
        out_shape=(
            jax.ShapeDtypeStruct((masters, width), jnp.bfloat16),
            jax.ShapeDtypeStruct(w_self.shape, jnp.float32),
            jax.ShapeDtypeStruct(w_neigh.shape, jnp.float32),
        ),
        in_specs=[VMEM] * 3,
        out_specs=[VMEM] * 3,
        compiler_params=pltpu.CompilerParams(vmem_limit_bytes=12 << 20),
        name="final",
    )(near(home), near(pre), near(weights))


def solution(mesh):
    placed = (
        P("dom", "feat"),
        P("dom", "feat"),
        P("dom", "feat"),
        P("dom", "feat"),
        P("feat", None),
        P("feat", None),
        P("dom"),
        P("dom"),
        P("dom"),
        P("dom"),
        P("dom"),
    )

    return jax.shard_map(
        on_device,
        mesh=mesh,
        in_specs=placed,
        out_specs=(P("dom", "feat"), P("feat", None), P("feat", None)),
        check_vma=False,
    )
```

```python
import functools

import jax
import jax.numpy as jnp
from jax import lax
from jax.experimental import pallas as pl
from jax.experimental.pallas import tpu as pltpu
from jax.sharding import PartitionSpec as P

LANES = 128
SUB = 8
GRID = (4, 8, 4)
CHAINS = 4
UNROLL = 8
VMEM = pl.BlockSpec(memory_space=pltpu.VMEM)
SMEM = pl.BlockSpec(memory_space=pltpu.SMEM)


def near(array):
    return pltpu.with_memory_space_constraint(array, pltpu.VMEM)


def far(array):
    return pltpu.with_memory_space_constraint(array, pltpu.HBM)


def ring(axis, shift):
    nx, nz, ny = GRID
    pairs = []
    for x in range(nx):
        for z in range(nz):
            for y in range(ny):
                tx = (x + shift) % nx if axis == "x" else x
                ty = (y + shift) % ny if axis == "y" else y
                pairs.append(((x * nz + z) * ny + y, (tx * nz + z) * ny + ty))
    return pairs


def columns():
    nx, nz, ny = GRID
    return [[(x * nz + z) * ny + y for z in range(nz)] for x in range(nx) for y in range(ny)]


def planes():
    nx, nz, ny = GRID
    return [[(x * nz + z) * ny + y for x in range(nx) for y in range(ny)] for z in range(nz)]


def swap(array, groups):
    return lax.all_to_all(array, "dom", split_axis=0, concat_axis=0, axis_index_groups=groups, tiled=True)


def sum_of(arrays):
    total = arrays[0].astype(jnp.float32)
    for a in arrays[1:]:
        total = total + a.astype(jnp.float32)
    return total


def picks_kernel(spot_ref, out_ref):
    groups, lanes = spot_ref.shape
    rows = out_ref.shape[2]

    def one(g, carry):
        spread = jnp.broadcast_to(spot_ref[pl.ds(g, 1), :].astype(jnp.float32), (LANES, lanes))
        across = jnp.concatenate([jnp.transpose(spread)] * (rows // min(rows, LANES)), axis=1)
        hub = lax.broadcasted_iota(jnp.int32, (lanes, across.shape[1]), 1).astype(jnp.float32)
        chosen = (across == hub).astype(jnp.float32).astype(jnp.bfloat16)
        out_ref[g] = chosen[:, 0:rows]
        return carry

    lax.fori_loop(0, groups, one, 0)


def edge_kernel(grid, slots, from_ref, to_ref, place_ref, own_ref, self_ref, spot_ref, pick_ref, *rest):
    nx, nz, ny = grid
    got_x = rest[0:ny]
    got_y = rest[ny : ny + nx]
    pre_ref = rest[ny + nx]
    back_x = rest[ny + nx + 1 : 2 * ny + nx + 1]
    back_y = rest[2 * ny + nx + 1 : 2 * (ny + nx) + 1]
    table = rest[2 * (ny + nx) + 1]
    sums = rest[2 * (ny + nx) + 2 :]
    masters, width = own_ref.shape
    halves = width // LANES
    tall = SUB * halves
    edges = from_ref.shape[0]
    deep = nz // 2

    def put(base, block):
        for g in range(block.shape[0] // SUB):
            for h in range(halves):
                at = pl.multiple_of(base + g * tall + h * SUB, SUB)
                table[pl.ds(at, SUB), :] = block[g * SUB : (g + 1) * SUB, h * LANES : (h + 1) * LANES]

    def own(i, carry):
        put(i * 32 * halves, own_ref[pl.ds(pl.multiple_of(i * 32, 32), 32), :].astype(jnp.float32))
        return carry

    lax.fori_loop(0, masters // 32, own, 0)

    def base_of(x, y, high, z):
        owner = (x * nz + high * deep + z) * ny + y
        return (masters + owner * slots) * halves

    def blocks(high, first, second):
        if high:
            x, y = place_ref[first], place_ref[nx + second]
        else:
            x, y = place_ref[second], place_ref[nx + first]
        return x, y, (x * ny + y) * 2 + high

    for high, got in ((0, got_x), (1, got_y)):
        for first in range(len(got)):

            def fetch(second, carry, high=high, first=first, got=got):
                x, y, group = blocks(high, first, second)
                rows = jnp.dot(pick_ref[group], got[first][second], preferred_element_type=jnp.float32)
                for z in range(deep):
                    put(base_of(x, y, high, z), rows[z * slots : (z + 1) * slots])
                return carry

            for second in range(got[first].shape[0]):
                fetch(second, 0)

    clear = 16 * SUB
    cleared = (masters + nx * nz * ny * slots) * halves

    def zero(i, carry):
        for s in sums:
            s[pl.ds(pl.multiple_of(i * clear, clear), clear), :] = jnp.zeros((clear, LANES), jnp.float32)
        return carry

    lax.fori_loop(0, cleared // clear, zero, 0)

    step = CHAINS * UNROLL

    def add(i, carry):
        for j in range(step):
            src = from_ref[i * step + j]
            dst = to_ref[i * step + j]
            into = sums[j % CHAINS]
            at = pl.ds(src, halves, stride=SUB)
            into[at, :] = into[at, :] + table[pl.ds(dst, halves, stride=SUB), :]
        return carry

    lax.fori_loop(0, edges // step, add, 0)

    def merged(base, rows, h):
        tiles = []
        for g in range(rows // SUB):
            at = pl.ds(pl.multiple_of(base + g * tall + h * SUB, SUB), SUB)
            value = sums[0][at, :]
            for s in sums[1:]:
                value = value + s[at, :]
            tiles.append(value)
        return jnp.concatenate(tiles, axis=0)

    def finish(i, carry):
        for h in range(halves):
            rows = pl.ds(pl.multiple_of(i * 32, 32), 32)
            cols = slice(h * LANES, (h + 1) * LANES)
            pre_ref[rows, cols] = self_ref[rows, cols] + merged(i * 32 * halves, 32, h)
        return carry

    lax.fori_loop(0, masters // 32, finish, 0)

    for high, back in ((0, back_x), (1, back_y)):
        for first in range(len(back)):
            for second in range(back[first].shape[0]):
                x, y, group = blocks(high, first, second)
                target = spot_ref[pl.ds(group, 1), :]
                rows = lax.broadcasted_iota(jnp.int32, (back[first].shape[1], target.shape[1]), 0)
                chosen = (rows == target).astype(jnp.float32).astype(jnp.bfloat16)
                block = jnp.concatenate(
                    [
                        jnp.concatenate(
                            [merged(base_of(x, y, high, z), slots, h) for h in range(halves)], axis=1
                        ).astype(jnp.bfloat16)
                        for z in range(deep)
                    ],
                    axis=0,
                )
                back[first][second] = jnp.dot(
                    chosen, block, preferred_element_type=jnp.float32
                ).astype(jnp.bfloat16)


def final_kernel(home_ref, pre_ref, weight_ref, grad_ref, self_ref, neigh_ref):
    hub = home_ref.shape[1]
    parts, pay, width = weight_ref.shape
    total = pre_ref[0:hub, :]
    for z in range(home_ref.shape[0]):
        total = total + home_ref[z].astype(jnp.float32)
    grad_ref[0:hub, :] = total.astype(jnp.bfloat16)
    grad_ref[hub:, :] = pre_ref[hub:, :].astype(jnp.bfloat16)
    quarter = parts // 4
    for which, ref in ((0, self_ref), (1, neigh_ref)):
        for half in range(2):

            def place(i, carry, which=which, ref=ref, half=half):
                peer = (which * 2 + half) * quarter + i
                rows = pl.ds(pl.multiple_of(i * pay, SUB), pay)
                ref[rows, half * width : (half + 1) * width] = weight_ref[peer].astype(jnp.float32)
                return carry

            lax.fori_loop(0, quarter, place, 0)


def on_device(
    features,
    grad_out,
    pre_act,
    neigh_mean,
    w_self,
    w_neigh,
    edge_from,
    edge_to,
    edge_count,
    mirror_master,
    degrees,
):
    nx, nz, ny = GRID
    deep = nz // 2
    masters, width = features.shape
    parts = lax.axis_size("dom")
    mirrors = mirror_master.shape[0]
    slots = mirrors // parts
    hub = min(masters, 64)
    local = masters + mirrors
    halves = width // LANES
    edges = edge_from.shape[0]
    contract = (((1,), (1,)), ((), ()))
    over_rows = (((0,), (0,)), ((), ()))
    first = lax.axis_index("feat") == 0

    def both(rows_out, rows_act):
        mine = (rows_out.astype(jnp.float32) * (rows_act > 0).astype(jnp.float32)).astype(jnp.bfloat16)
        other = lax.ppermute(mine, "feat", [(0, 1), (1, 0)])
        return jnp.concatenate([jnp.where(first, mine, other), jnp.where(first, other, mine)], axis=1)

    def scale(cols, degree):
        part = lax.dot_general(cols, w_neigh, contract, preferred_element_type=jnp.float32)
        return (part / degree[:, None].astype(jnp.float32)).astype(jnp.bfloat16)

    shared = scale(both(grad_out[:hub], pre_act[:hub]), degrees[:hub])
    copies = jnp.broadcast_to(shared, (nz, *shared.shape))
    column = lax.all_to_all(
        copies, "dom", split_axis=0, concat_axis=0, axis_index_groups=columns(), tiled=True
    )

    block_cols = both(grad_out, pre_act)
    grad_self = lax.dot_general(features, block_cols, over_rows, preferred_element_type=jnp.float32)
    grad_neigh = lax.dot_general(neigh_mean, block_cols, over_rows, preferred_element_type=jnp.float32)
    pay = jnp.concatenate(
        [grad_self[:, :width], grad_self[:, width:], grad_neigh[:, :width], grad_neigh[:, width:]],
        axis=0,
    ).astype(jnp.bfloat16)
    tail = pay.shape[0] // parts

    low = column[:deep].reshape(deep * hub, width)
    high = column[deep:].reshape(deep * hub, width)
    low_far = [lax.ppermute(low, "dom", ring("x", k)) for k in range(1, nx)]
    high_far = [lax.ppermute(high, "dom", ring("y", k)) for k in range(1, ny)]
    pieces = swap(pay.reshape(nz, -1, width), columns())
    low_set = jnp.stack([low] + low_far)
    high_set = jnp.stack([high] + high_far)
    low_got = [low_set] + [lax.ppermute(low_set, "dom", ring("y", k)) for k in range(1, ny)]
    high_got = [high_set] + [lax.ppermute(high_set, "dom", ring("x", k)) for k in range(1, nx)]
    scaled = scale(block_cols, degrees)
    self_part = lax.dot_general(block_cols, w_self, contract, preferred_element_type=jnp.float32)
    chunk = jnp.sum(pieces.astype(jnp.float32), axis=0).astype(jnp.bfloat16)
    chunks = jnp.broadcast_to(chunk, (nx * ny, *chunk.shape))
    chunks = swap(chunks, planes())

    order = mirror_master.reshape(nx, 2, deep, ny, slots).transpose(0, 3, 1, 2, 4)
    spots = order.reshape(nx * ny * 2, deep * slots) + jnp.repeat(
        jnp.arange(deep, dtype=jnp.int32) * hub, slots
    )
    chosen = pl.pallas_call(
        picks_kernel,
        out_shape=pltpu.VMEM((nx * ny * 2, deep * slots, deep * hub), jnp.bfloat16),
        in_specs=[VMEM],
        out_specs=VMEM,
        compiler_params=pltpu.CompilerParams(vmem_limit_bytes=8 << 20),
        name="picks",
    )(spots)

    def spot(row):
        return (row // SUB) * (SUB * halves) + row % SUB

    live = jnp.arange(edges, dtype=jnp.int32) < edge_count[0]
    from_at = spot(jnp.where(live, edge_from, local))
    to_at = spot(edge_to)
    me = lax.axis_index("dom")
    my_x, my_y = me // (nz * ny), me % ny
    place = jnp.concatenate(
        [(my_x - jnp.arange(nx, dtype=jnp.int32)) % nx, (my_y - jnp.arange(ny, dtype=jnp.int32)) % ny]
    ).astype(jnp.int32)

    lanes = local * halves
    spare = SUB * SUB
    low_type = pltpu.HBM(low_set.shape, jnp.bfloat16)
    high_type = pltpu.HBM(high_set.shape, jnp.bfloat16)
    edge_call = pl.pallas_call(
        functools.partial(edge_kernel, GRID, slots),
        out_shape=[pltpu.HBM((masters, width), jnp.float32)] + [low_type] * ny + [high_type] * nx,
        in_specs=[SMEM] * 3 + [VMEM] * (4 + nx + ny),
        out_specs=[VMEM] * (1 + nx + ny),
        scratch_shapes=[pltpu.VMEM((lanes + spare, LANES), jnp.float32)]
        + [pltpu.VMEM((lanes + SUB * halves + spare, LANES), jnp.float32) for _ in range(CHAINS)],
        compiler_params=pltpu.CompilerParams(vmem_limit_bytes=42 << 20),
        name="edges",
    )
    results = edge_call(from_at, to_at, place, far(scaled), far(self_part), near(spots), near(chosen), *low_got, *high_got)
    pre, low_back, high_back = results[0], results[1 : 1 + ny], results[1 + ny :]

    share = jnp.sum(chunks.astype(jnp.float32), axis=0).astype(jnp.bfloat16)
    low_part = [low_back[0]] + [lax.ppermute(low_back[k], "dom", ring("y", -k)) for k in range(1, ny)]
    high_part = [high_back[0]] + [lax.ppermute(high_back[k], "dom", ring("x", -k)) for k in range(1, nx)]
    weights = swap(jnp.broadcast_to(share, (nz, *share.shape)), columns()).reshape(parts, tail, width)
    low_sum = [sum_of([p[k] for p in low_part]) for k in range(nx)]
    high_sum = [sum_of([p[k] for p in high_part]) for k in range(ny)]
    low_sent = [low_sum[0]] + [
        lax.ppermute(low_sum[k].astype(jnp.bfloat16), "dom", ring("x", -k)) for k in range(1, nx)
    ]
    high_sent = [high_sum[0]] + [
        lax.ppermute(high_sum[k].astype(jnp.bfloat16), "dom", ring("y", -k)) for k in range(1, ny)
    ]
    column_sum = jnp.concatenate([sum_of(low_sent), sum_of(high_sent)], axis=0).astype(jnp.bfloat16)
    column_sum, weights, pre = lax.optimization_barrier((column_sum, weights, pre))
    home = lax.all_to_all(
        column_sum.reshape(nz, hub, width),
        "dom",
        split_axis=0,
        concat_axis=0,
        axis_index_groups=columns(),
        tiled=True,
    )
    return pl.pallas_call(
        final_kernel,
        out_shape=(
            jax.ShapeDtypeStruct((masters, width), jnp.bfloat16),
            jax.ShapeDtypeStruct(w_self.shape, jnp.float32),
            jax.ShapeDtypeStruct(w_neigh.shape, jnp.float32),
        ),
        in_specs=[VMEM] * 3,
        out_specs=[VMEM] * 3,
        compiler_params=pltpu.CompilerParams(vmem_limit_bytes=12 << 20),
        name="final",
    )(near(home), near(pre), near(weights))


def solution(mesh):
    placed = (
        P("dom", "feat"),
        P("dom", "feat"),
        P("dom", "feat"),
        P("dom", "feat"),
        P("feat", None),
        P("feat", None),
        P("dom"),
        P("dom"),
        P("dom"),
        P("dom"),
        P("dom"),
    )

    return jax.shard_map(
        on_device,
        mesh=mesh,
        in_specs=placed,
        out_specs=(P("dom", "feat"), P("feat", None), P("feat", None)),
        check_vma=False,
    )
```
